32 devices in a mesh: tower: 2 (over x), dp: 16 (over z, y, core).
Axes of the slice: x: 2, y: 2, z: 4, core: 2. Of those that a mesh axis runs over, the one named last changes fastest.
Arguments:
- images: bfloat16 [288, 50, 768], P('dp'), may hold values from -6 to 6
- captions: bfloat16 [864, 16, 768], P('dp'), may hold values from -6 to 6
- token_ids: int32 [864, 16], P('dp'), may hold values from 0 to 31999, as said below
- counts: int32 [288], P('dp'), may hold values from 1 to 5, as said below
- matches: int32 [864], P('dp'), may hold values from 0 to 287, as said below
- image_weights: bfloat16 [9216, 768], P('dp')
- image_norms: float32 [4, 768], replicated, may hold values from -1.2 to 1.2, as said below
- weights: float32 [9216, 768], P(('tower', 'dp'))
- norm_params: float32 [4, 768], replicated, may hold values from -1.2 to 1.2, as said below
- momentum: float32 [9216, 768], P(('tower', 'dp'))
- norm_momentum: float32 [4, 768], replicated
- averages: float32 [9216, 768], P(('tower', 'dp'))
- norm_averages: float32 [4, 768], replicated, may hold values from -1.2 to 1.2
Outputs:
- grads: float32 [9216, 768], P(('tower', 'dp'))
- norm_grads: float32 [4, 768], replicated
- input_grad: float32 [864, 16, 768], P('dp', None, 'tower')
- new_weights: float32 [9216, 768], P(('tower', 'dp'))
- new_momentum: float32 [9216, 768], P(('tower', 'dp'))
- new_averages: float32 [9216, 768], P(('tower', 'dp'))
- new_norm_params: float32 [4, 768], replicated
- new_norm_momentum: float32 [4, 768], replicated
- new_norm_averages: float32 [4, 768], replicated
- grad_norm: float32 [], replicated
The draws below stay inside these ranges and needn't reach their ends.
Inputs may be any that keep to these rules, and one draw needn't show every extreme that they name: `token_ids`: in each caption the ids are nonzero on a leading run of 4 to 16 positions and 0 after it. counts[i] is the number of captions c with matches[c] = i; the counts sum to 864. `matches`: image i is named by exactly counts[i] captions. `norm_params`: rows 0 and 2 are gains, rows 1 and 3 biases. `image_norms`: rows 0 and 2 are gains, rows 1 and 3 biases.
All inputs are finite; a program needn't handle non-finite values.
Results may differ from the reference program's by a relative error of at most 0.014.
The reference program's roundings to bfloat16 on the way count: a program that leaves them out, or rounds other values in their place, can miss the bound.
Values may be sent and summed in bfloat16 or wider, within the bound.
No kernel may reach another device: no remote copies, remote signals or barrier semaphores. Data moves between devices by JAX's collectives and lax.ppermute only.
A program may use at most 320 MiB of HBM per device.

```python
import math
import jax
import jax.numpy as jnp
from jax import lax

D = 768
HEADS = 12
HEAD_DIM = 64
FF = 3072
IMG_ROWS = 50
TXT_LEN = 16
VOCAB = 32000
IMG_DEV = 18
CAP_DEV = 54
IMAGES = 288
CAPTIONS = 864
WROWS = 9216
N_DP = 16


def pair_counts(key):
    base_key = jax.random.fold_in(key, 11)
    first_key, order_key, shuffle_key = jax.random.split(base_key, 3)
    halves = jax.random.randint(first_key, (IMAGES // 2,), 1, 6)
    halves = halves.at[0].set(5)
    placed = jnp.stack([halves, 6 - halves], axis=1).reshape(IMAGES)
    ordering = jax.random.permutation(order_key, IMAGES)
    counts = jnp.zeros((IMAGES,), jnp.int32).at[ordering].set(placed.astype(jnp.int32))
    return (counts, shuffle_key)


def draw_counts(key, part):
    return pair_counts(key)[0]


def draw_matches(key, part):
    counts, shuffle_key = pair_counts(key)
    listed = jnp.repeat(jnp.arange(IMAGES, dtype=jnp.int32), counts, total_repeat_length=CAPTIONS)
    return listed[jax.random.permutation(shuffle_key, CAPTIONS)]


def draw_token_ids(key, part):
    length_key, word_key = jax.random.split(jax.random.fold_in(key, 23))
    lengths = jax.random.randint(length_key, (CAPTIONS,), 4, TXT_LEN + 1)
    lengths = lengths.at[0].set(TXT_LEN).at[1].set(4)
    words = jax.random.randint(word_key, (CAPTIONS, TXT_LEN), 1, VOCAB)
    words = words.at[0, 0].set(VOCAB - 1)
    places = jnp.arange(TXT_LEN)[None, :]
    return jnp.where(places < lengths[:, None], words, 0).astype(jnp.int32)


def row_scales(attention_gain):
    rows_index = jnp.arange(WROWS)
    first = D ** (-0.5)
    return jnp.where(rows_index < 3 * D, first, jnp.where(rows_index < 4 * D, attention_gain * first, jnp.where(rows_index < 4 * D + FF, first, FF ** (-0.5))))


def matrix_draw(key, stream, attention_gain):
    sample_key = jax.random.fold_in(key, stream)
    sample = jnp.clip(jax.random.normal(sample_key, (WROWS, D), jnp.float32), -4.0, 4.0)
    return sample * row_scales(attention_gain)[:, None]


def draw_weights(key, part):
    return matrix_draw(key, 31, 2.5)


def draw_image_weights(key, part):
    return matrix_draw(key, 37, 4.0).astype(jnp.bfloat16)


def draw_averages(key, part):
    return matrix_draw(key, 41, 2.5)


def norm_rows(key, stream):
    gain_key, shift_key = jax.random.split(jax.random.fold_in(key, stream))
    gain_rows = 1.0 + 0.15 * jax.random.uniform(gain_key, (2, D), jnp.float32, -1.0, 1.0)
    shifts = 0.3 * jnp.clip(jax.random.normal(shift_key, (2, D), jnp.float32), -4.0, 4.0)
    return jnp.stack([gain_rows[0], shifts[0], gain_rows[1], shifts[1]])


def draw_image_norms(key, part):
    return norm_rows(key, 43)


def draw_norm_params(key, part):
    return norm_rows(key, 47)


def draw_norm_averages(key, part):
    return norm_rows(key, 53)


def draw_momentum(key, part):
    sample = jax.random.normal(jax.random.fold_in(key, 59), (WROWS, D), jnp.float32)
    return sample * (1.1 / math.sqrt(WROWS * D))


def draw_norm_momentum(key, part):
    sample = jax.random.normal(jax.random.fold_in(key, 61), (4, D), jnp.float32)
    return sample * (3.0 / math.sqrt(WROWS * D))


def level_of(key, dims, shards, smallest, largest):
    level, own = 1.0, jax.random.fold_in(key, 6)
    for dim, shards_of in shards:
        steps = jnp.exp(jax.random.uniform(jax.random.fold_in(own, dim), (shards_of,), jnp.float32, smallest / len(shards), largest / len(shards)))
        level = level * jnp.repeat(steps, dims[dim] // shards_of).reshape([-1 if axis == dim else 1 for axis in range(len(dims))])
    return level


def bell_draw(key, dims, deviation, most, shards=(), kind=jnp.bfloat16):
    factor_of = level_of(key, dims, shards, -0.22, 0.18) if shards else 1.0
    drawn = jax.random.normal(key, dims, jnp.float32) * deviation * factor_of
    return jnp.minimum(jnp.maximum(drawn, -most), most).astype(kind)


def setup_inputs(seed: int = 0) -> dict:
    keys = jax.random.split(jax.random.key(seed), 14)
    images = bell_draw(keys[0], (IMAGES, IMG_ROWS, D), 1.0, 6.0, ((0, 16),))
    captions = bell_draw(keys[1], (CAPTIONS, TXT_LEN, D), 1.0, 6.0, ((0, 16),))
    token_ids = draw_token_ids(jax.random.fold_in(keys[13], 71), 0)
    counts = draw_counts(jax.random.fold_in(keys[13], 71), 0)
    matches = draw_matches(jax.random.fold_in(keys[13], 71), 0)
    image_weights = draw_image_weights(jax.random.fold_in(keys[13], 71), 0)
    image_norms = draw_image_norms(jax.random.fold_in(keys[13], 71), 0)
    weights = draw_weights(jax.random.fold_in(keys[13], 71), 0)
    norm_params = draw_norm_params(jax.random.fold_in(keys[13], 71), 0)
    momentum = draw_momentum(jax.random.fold_in(keys[13], 71), 0)
    norm_momentum = draw_norm_momentum(jax.random.fold_in(keys[13], 71), 0)
    averages = draw_averages(jax.random.fold_in(keys[13], 71), 0)
    norm_averages = draw_norm_averages(jax.random.fold_in(keys[13], 71), 0)
    return {"images": images, "captions": captions, "token_ids": token_ids, "counts": counts, "matches": matches, "image_weights": image_weights, "image_norms": image_norms, "weights": weights, "norm_params": norm_params, "momentum": momentum, "norm_momentum": norm_momentum, "averages": averages, "norm_averages": norm_averages}


@jax.custom_vjp
def low(v):
    return lax.optimization_barrier(v.astype(jnp.bfloat16)).astype(jnp.float32)

@jax.custom_vjp
def low_back(v):
    return v

def low_keep(v):
    return (low(v), None)

def low_pass(kept, grad):
    return (grad,)

def back_keep(v):
    return (v, None)

def back_low(kept, grad):
    return (low(grad),)
low.defvjp(low_keep, low_pass)
low_back.defvjp(back_keep, back_low)
EPSILON = 1e-06
LOGIT_SCALE = 50.0
CLIP_NORM = 1.0
MOMENTUM_RATE = 0.9
DECAY_RATE = 0.0001
AVERAGE_RATE = 0.7

def layer_norm(rows_in, scaling, offset):
    middle = lax.optimization_barrier(jnp.mean(rows_in, axis=-1, keepdims=True))
    centred = rows_in - middle
    spread = lax.optimization_barrier(jnp.mean(centred * centred, axis=-1, keepdims=True))
    return centred * lax.rsqrt(spread + EPSILON) * scaling + offset

def product(left, right):
    return jnp.einsum('...k,nk->...n', left, right, precision=lax.Precision.HIGHEST)

def block_forward(rows_in, packed, norms, causal):
    features = rows_in.shape[-1]
    hidden_units = (packed.shape[0] - 4 * features) // 2
    qkv_matrix = packed[:3 * features]
    out_matrix = packed[3 * features:4 * features]
    up_matrix = packed[4 * features:4 * features + hidden_units]
    down_matrix = packed[4 * features + hidden_units:]
    seq_count, seq_length = (rows_in.shape[0], rows_in.shape[1])
    normed = low(layer_norm(rows_in, norms[0], norms[1]))
    joined = low(product(normed, qkv_matrix)).reshape(seq_count, seq_length, 3, HEADS, HEAD_DIM)
    queries = low_back(joined[:, :, 0])
    key_rows = low_back(joined[:, :, 1])
    values = low_back(joined[:, :, 2])
    scores = low_back(jnp.einsum('nqhd,nkhd->nhqk', queries, key_rows, precision=lax.Precision.HIGHEST)) * HEAD_DIM ** (-0.5)
    if causal:
        causal_mask = jnp.arange(seq_length)[:, None] >= jnp.arange(seq_length)[None, :]
        scores = jnp.where(causal_mask, scores, -1e+30)
    attn_probs = low(jax.nn.softmax(scores, axis=-1))
    attended = jnp.einsum('nhqk,nkhd->nqhd', attn_probs, values, precision=lax.Precision.HIGHEST)
    attended = low(low_back(attended.reshape(seq_count, seq_length, features)))
    hidden = rows_in + low_back(product(attended, out_matrix))
    normed_mid = low(layer_norm(hidden, norms[2], norms[3]))
    pre_act = low_back(product(normed_mid, up_matrix))
    activated = low(low_back(jax.nn.gelu(pre_act, approximate=True)))
    return hidden + low_back(jnp.einsum('nlf,fd->nld', activated, down_matrix, precision=lax.Precision.HIGHEST))

def image_embed(images_group, frozen, image_norms):
    block_out = block_forward(images_group.astype(jnp.float32), frozen, image_norms, False)
    top_rows = block_out[:, 0]
    return low(top_rows * lax.rsqrt(lax.optimization_barrier(jnp.sum(top_rows * top_rows, axis=-1, keepdims=True)) + EPSILON))

def text_embed(packed, norms, tokens, token_ids):
    block_out = block_forward(tokens, low(packed), norms, True)
    lengths = lax.optimization_barrier(jnp.sum((token_ids != 0).astype(jnp.int32), axis=1))
    pool_mask = (jnp.arange(TXT_LEN, dtype=jnp.int32)[None, :] == (lengths - 1)[:, None]).astype(block_out.dtype)
    pooled = lax.optimization_barrier(jnp.sum(block_out * pool_mask[:, :, None], axis=1))
    return low(pooled * lax.rsqrt(lax.optimization_barrier(jnp.sum(pooled * pooled, axis=-1, keepdims=True)) + EPSILON))

def contrast(text_emb, image_emb, matches, counts):
    logits = LOGIT_SCALE * low_back(product(text_emb, image_emb))
    target = (matches[:, None] == jnp.arange(image_emb.shape[0], dtype=jnp.int32)[None, :]).astype(logits.dtype)
    row_part = jnp.sum(jax.nn.logsumexp(logits, axis=1)) - jnp.sum(logits * target)
    column_part = jnp.sum(jax.nn.logsumexp(logits, axis=0)) - jnp.sum(logits * target / counts.astype(logits.dtype)[None, :])
    return 0.5 * (row_part + column_part)

def reference(images, captions, token_ids, counts, matches, image_weights, image_norms, weights, norm_params, momentum, norm_momentum, averages, norm_averages):
    frozen = image_weights.astype(jnp.float32)
    image_groups = images.reshape(N_DP // 2, 2 * IMG_DEV, IMG_ROWS, D)

    def embed_images(image_group):
        return image_embed(image_group, frozen, image_norms)
    image_emb = lax.map(embed_images, image_groups).reshape(IMAGES, D)
    caption_groups = captions.reshape(N_DP // 2, 2 * CAP_DEV, TXT_LEN, D)
    id_groups = token_ids.reshape(N_DP // 2, 2 * CAP_DEV, TXT_LEN)

    def embed_captions(caption_pair):
        return text_embed(weights, norm_params, caption_pair[0].astype(jnp.float32), caption_pair[1])
    text_emb = lax.map(embed_captions, (caption_groups, id_groups)).reshape(CAPTIONS, D)
    grad_embed = jax.grad(contrast)(text_emb, image_emb, matches, counts).reshape(N_DP // 2, 2 * CAP_DEV, D)

    def one_group(totals, slices):
        tokens, group_ids, cotangent = slices

        def local_embed(packed, norms, rows_in):
            return text_embed(packed, norms, rows_in, group_ids)
        pull = jax.vjp(local_embed, weights, norm_params, tokens.astype(jnp.float32))[1]
        grad_w, grad_n, grad_x = pull(cotangent)
        return ((totals[0] + grad_w, totals[1] + grad_n), grad_x)
    start = (jnp.zeros_like(weights), jnp.zeros_like(norm_params))
    (raw_grads, raw_norm_grads), input_parts = lax.scan(one_group, start, (caption_groups, id_groups, grad_embed))
    input_grad = input_parts.reshape(CAPTIONS, TXT_LEN, D)
    grad_norm = jnp.sqrt(jnp.sum(raw_grads * raw_grads) + jnp.sum(raw_norm_grads * raw_norm_grads))
    factor = jnp.minimum(1.0, CLIP_NORM / (grad_norm + 1e-06))
    grads = raw_grads * factor
    norm_grads = raw_norm_grads * factor
    step_rate = 0.4 * math.sqrt(WROWS)
    decayed = grads + DECAY_RATE * weights
    new_momentum = MOMENTUM_RATE * momentum + decayed
    new_weights = weights - step_rate * (decayed + MOMENTUM_RATE * new_momentum)
    new_averages = AVERAGE_RATE * averages + (1.0 - AVERAGE_RATE) * new_weights
    new_norm_momentum = MOMENTUM_RATE * norm_momentum + norm_grads
    new_norm_params = norm_params - step_rate * (norm_grads + MOMENTUM_RATE * new_norm_momentum)
    new_norm_averages = AVERAGE_RATE * norm_averages + (1.0 - AVERAGE_RATE) * new_norm_params
    return (grads, norm_grads, input_grad, new_weights, new_momentum, new_averages, new_norm_params, new_norm_momentum, new_norm_averages, grad_norm)
```

```python
from functools import partial
import math

import jax
import jax.numpy as jnp
import numpy as np
from jax import lax
from jax.experimental import pallas as pl
from jax.experimental.pallas import tpu as pltpu
from jax.sharding import PartitionSpec as P

HEAD_DIM = 64
GROUP = 4

EPSILON = 1e-06
LOGIT_SCALE = 50.0
CLIP_NORM = 1.0
MOMENTUM_RATE = 0.9
DECAY_RATE = 0.0001
AVERAGE_RATE = 0.7
MASKED = -1e30
GELU_A = 0.044715
GELU_C = math.sqrt(2.0 / math.pi)

f32 = jnp.float32
bf16 = jnp.bfloat16


def round_up(value, step):
    return (value + step - 1) // step * step


def dot_nn(left, right, **kw):
    return lax.dot_general(
        left, right, (((1,), (0,)), ((), ())), preferred_element_type=f32, **kw
    )


def dot_nt(left, right):
    return lax.dot_general(left, right, (((1,), (1,)), ((), ())), preferred_element_type=f32)


def dot_tn(left, right):
    return lax.dot_general(left, right, (((0,), (0,)), ((), ())), preferred_element_type=f32)


def call(kernel, outs, *args, scratch=(), name=None, flops=0):
    whole = pl.BlockSpec(memory_space=pltpu.VMEM)
    return pl.pallas_call(
        kernel,
        out_shape=outs,
        in_specs=[whole] * len(args),
        out_specs=jax.tree.map(lambda _: whole, outs),
        scratch_shapes=list(scratch),
        name=name,
    )(*args)


def sds(shape, dtype):
    return jax.ShapeDtypeStruct(shape, dtype)


def normalize(rows):
    middle = jnp.mean(rows, axis=-1, keepdims=True)
    centred = rows - middle
    spread = jnp.mean(centred * centred, axis=-1, keepdims=True)
    scale = lax.rsqrt(spread + EPSILON)
    return centred * scale, scale


def norm_pull(grad, rows, gain):
    unit, scale = normalize(rows)
    scaled = grad * gain
    pulled = scale * (
        scaled
        - jnp.mean(scaled, axis=-1, keepdims=True)
        - unit * jnp.mean(scaled * unit, axis=-1, keepdims=True)
    )
    return pulled, grad * unit


def lanes_of_heads(count):
    return lax.broadcasted_iota(jnp.int32, (count, GROUP * HEAD_DIM), 1) // HEAD_DIM


def stack_heads(block):
    lanes = lanes_of_heads(block.shape[0])
    zero = jnp.zeros_like(block)
    return jnp.concatenate([jnp.where(lanes == h, block, zero) for h in range(GROUP)], axis=0)


def unstack_heads(block):
    count = block.shape[0] // GROUP
    lanes = lanes_of_heads(count)
    total = jnp.where(lanes == 0, block[:count], 0.0)
    for h in range(1, GROUP):
        total = jnp.where(lanes == h, block[h * count : (h + 1) * count], total)
    return total


def group_slice(index, base=0):
    return pl.ds(pl.multiple_of(base + index * 256, 256), 256)


def rows_kernel(step, x_ref, pos_ref, norms_ref, normed_ref, npool_ref, xpool_ref):
    gain, offset = norms_ref[0:1, :], norms_ref[1:2, :]

    @pl.loop(0, x_ref.shape[0] // step)
    def _(i):
        here = pl.ds(pl.multiple_of(i * step, step), step)
        unit, _ = normalize(x_ref[here, :].astype(f32))
        normed_ref[here, :] = (unit * gain + offset).astype(bf16)

    count = npool_ref.shape[0]
    pick = (
        lax.broadcasted_iota(jnp.int32, (count, x_ref.shape[0]), 1) == pos_ref[...]
    ).astype(bf16)
    npool_ref[...] = dot_nn(pick, normed_ref[...]).astype(bf16)
    xpool_ref[...] = dot_nn(pick, x_ref[...])


def attend_kernel(
    normed_ref, npool_ref, xpool_ref, norms_ref, low_ref, high_ref, w_ref,
    q_ref, k_ref, v_ref, probs_ref, att_ref, hidden_ref, nm_ref,
):
    count, features = npool_ref.shape
    total = normed_ref.shape[0]
    keys = lax.broadcasted_iota(jnp.int32, (count, total), 1)
    allowed = ((keys >= low_ref[...]) & (keys < high_ref[...]))[None]

    @pl.loop(0, features // 256)
    def _(i):
        cols = group_slice(i)
        queries = dot_nt(npool_ref[...], w_ref[group_slice(i), :]).astype(bf16)
        key_rows = dot_nt(normed_ref[...], w_ref[group_slice(i, features), :]).astype(bf16)
        values = dot_nt(normed_ref[...], w_ref[group_slice(i, 2 * features), :]).astype(bf16)
        q_ref[:, cols] = queries
        k_ref[:, cols] = key_rows
        v_ref[:, cols] = values
        scores = dot_nt(stack_heads(queries), key_rows) * HEAD_DIM**-0.5
        scores = jnp.where(allowed, scores.reshape(GROUP, count, total), MASKED)
        exponent = jnp.exp(scores - jnp.max(scores, axis=-1, keepdims=True))
        probs = exponent / jnp.sum(exponent, axis=-1, keepdims=True)
        probs = probs.reshape(GROUP * count, total)
        probs_ref[i] = probs
        att_ref[:, cols] = unstack_heads(dot_nn(probs.astype(bf16), values)).astype(bf16)

    hidden = xpool_ref[...] + dot_nt(
        att_ref[...], w_ref[pl.ds(3 * features, features), :]
    )
    hidden_ref[...] = hidden
    unit, _ = normalize(hidden)
    nm_ref[...] = (unit * norms_ref[2:3, :] + norms_ref[3:4, :]).astype(bf16)


def gelu_parts(pre):
    tanh = jnp.tanh(GELU_C * (pre + GELU_A * pre * pre * pre))
    return 0.5 * (1.0 + tanh), tanh


def feed_kernel(
    nm_ref, hidden_ref, up_ref, down_ref,
    pre_ref, act_ref, pooled_ref, inverse_ref, emb_ref, total_ref,
):
    step = pl.program_id(0)
    pre = dot_nt(nm_ref[...], up_ref[...])
    pre_ref[...] = pre
    act = (pre * gelu_parts(pre)[0]).astype(bf16)
    act_ref[...] = act
    part = dot_nn(act, down_ref[...])

    @pl.when(step == 0)
    def _():
        total_ref[...] = part

    @pl.when(step > 0)
    def _():
        total_ref[...] += part

    @pl.when(step == pl.num_programs(0) - 1)
    def _():
        pooled = hidden_ref[...] + total_ref[...]
        inverse = lax.rsqrt(jnp.sum(pooled * pooled, axis=-1, keepdims=True) + EPSILON)
        pooled_ref[...] = pooled
        inverse_ref[...] = jnp.broadcast_to(inverse, inverse_ref.shape)
        emb_ref[...] = (pooled * inverse).astype(bf16)


def loss_kernel(
    chunk, slots, text_ref, img_ref, row_bias_ref, col_bias_ref, emb_ref, pooled_ref, inverse_ref,
    place_ref, count_place_ref, slot_ref, real_ref, grad_ref, branch_ref,
):
    images = img_ref.shape[0]
    count = emb_ref.shape[0]

    def body(j, carry):
        top, acc = carry
        here = pl.ds(pl.multiple_of(j * chunk, chunk), chunk)
        logits = LOGIT_SCALE * dot_nt(text_ref[here, :], img_ref[...]) + row_bias_ref[here, :]
        higher = jnp.maximum(top, jnp.max(logits, axis=0, keepdims=True))
        acc = acc * jnp.exp(top - higher) + jnp.sum(
            jnp.exp(logits - higher), axis=0, keepdims=True
        )
        return higher, acc

    top, acc = lax.fori_loop(
        0,
        text_ref.shape[0] // chunk,
        body,
        (jnp.full((1, images), MASKED, f32), jnp.zeros((1, images), f32)),
    )
    column_lse = top + jnp.log(acc)
    logits = LOGIT_SCALE * dot_nt(emb_ref[...], img_ref[...])
    masked = logits + col_bias_ref[...]
    row_top = jnp.max(masked, axis=1, keepdims=True)
    row_exp = jnp.exp(masked - row_top)
    by_row = row_exp / jnp.sum(row_exp, axis=1, keepdims=True)
    by_column = jnp.exp(masked - column_lse)
    columns = lax.broadcasted_iota(jnp.int32, (count, images), 1)
    target = (columns == place_ref[...]).astype(f32)
    listed = dot_nn((columns == count_place_ref[...]).astype(bf16), img_ref[...])
    at = lax.broadcasted_iota(jnp.int32, listed.shape, 1) == slot_ref[...]
    named = jnp.maximum(jnp.sum(jnp.where(at, listed, 0.0), axis=1, keepdims=True), 1.0)
    grad_logits = 0.5 * (by_row - target) + 0.5 * (by_column - target / named)
    scaled = jnp.where(
        (col_bias_ref[...] == 0.0) & (real_ref[...] > 0.0), LOGIT_SCALE * grad_logits, 0.0
    ).astype(bf16)
    grad_embed = dot_nn(scaled, img_ref[...])
    pooled = pooled_ref[...]
    inverse = inverse_ref[:, 0:1]
    projection = jnp.sum(pooled * grad_embed, axis=-1, keepdims=True)
    grad_pooled = inverse * grad_embed - inverse * inverse * inverse * projection * pooled
    grad_ref[...] = grad_pooled
    branch_ref[...] = grad_pooled.astype(bf16)


def feed_back_kernel(
    branch_ref, grad_ref, hidden_ref, norms_ref, pre_ref, up_ref, down_ref,
    gpre_ref, ghidden_ref, mixed_ref, sums_ref, total_ref,
):
    step = pl.program_id(0)
    pre = pre_ref[...]
    cdf, tanh = gelu_parts(pre)
    slope = cdf + pre * 0.5 * (1.0 - tanh * tanh) * GELU_C * (1.0 + 3.0 * GELU_A * pre * pre)
    grad_act = dot_nt(branch_ref[...], down_ref[...]).astype(bf16)
    gpre = (grad_act.astype(f32) * slope).astype(bf16)
    gpre_ref[...] = gpre
    part = dot_nn(gpre, up_ref[...])

    @pl.when(step == 0)
    def _():
        total_ref[...] = part

    @pl.when(step > 0)
    def _():
        total_ref[...] += part

    @pl.when(step == pl.num_programs(0) - 1)
    def _():
        grad = total_ref[...]
        pulled, by_gain = norm_pull(grad, hidden_ref[...], norms_ref[2:3, :])
        ghidden = grad_ref[...] + pulled
        ghidden_ref[...] = ghidden
        mixed_ref[...] = ghidden.astype(bf16)
        sums_ref[...] = jnp.zeros_like(sums_ref)
        sums_ref[2:3, :] = jnp.sum(by_gain, axis=0, keepdims=True)
        sums_ref[3:4, :] = jnp.sum(grad, axis=0, keepdims=True)


def attend_back_kernel(
    step, half, mixed_ref, ghidden_ref, probs_ref, q_ref, k_ref, v_ref, x_ref, pos_ref, norms_ref,
    sums_in_ref, fold_ref, w_ref,
    gatt_ref, gq_ref, craw_ref, cprob_ref, left_ref, right_ref, sums_ref, grad_ref,
):
    count, features = mixed_ref.shape
    gatt_ref[...] = dot_nn(mixed_ref[...], w_ref[pl.ds(3 * features, features), :]).astype(bf16)

    @pl.loop(0, features // 256)
    def _(i):
        cols = group_slice(i)
        gatt = stack_heads(gatt_ref[:, cols])
        queries = stack_heads(q_ref[:, cols])
        key_rows, values = k_ref[:, cols], v_ref[:, cols]
        probs = probs_ref[i]
        grad_probs = dot_nt(gatt, values)
        mean = jnp.sum(probs * grad_probs, axis=-1, keepdims=True)
        raw = (probs * (grad_probs - mean) * HEAD_DIM**-0.5).astype(bf16)
        low = probs.astype(bf16)
        gq_ref[:, cols] = unstack_heads(dot_nn(raw, key_rows)).astype(bf16)
        gk = dot_tn(raw, queries).astype(bf16)
        gv = dot_tn(low, gatt).astype(bf16)
        part = dot_nn(gk, w_ref[group_slice(i, features), :]) + dot_nn(
            gv, w_ref[group_slice(i, 2 * features), :]
        )

        @pl.when(i == 0)
        def _():
            grad_ref[...] = part

        @pl.when(i > 0)
        def _():
            grad_ref[...] += part

        fold = fold_ref[...]
        craw_ref[i] = lax.dot_general(
            fold, raw, (((0,), (1,)), ((), ())), preferred_element_type=f32
        ).astype(bf16)
        cprob_ref[i] = lax.dot_general(
            fold, low, (((0,), (1,)), ((), ())), preferred_element_type=f32
        ).astype(bf16)

    gpool = dot_nn(gq_ref[...], w_ref[pl.ds(0, features), :])
    gain = norms_ref[0:1, :]

    def body(j, carry):
        dgain, doffset = carry
        here = pl.ds(pl.multiple_of(j * step, step), step)
        pick = (
            lax.broadcasted_iota(jnp.int32, (step, count), 0) + j * step == pos_ref[...]
        ).astype(f32)
        grad = grad_ref[here, :] + dot_nn(pick, gpool, precision=lax.Precision.HIGHEST)
        pulled, by_gain = norm_pull(grad, x_ref[here, :].astype(f32), gain)
        pulled = pulled + dot_nn(pick, ghidden_ref[...], precision=lax.Precision.HIGHEST)
        left_ref[here, :] = pulled[:, :half].astype(bf16)
        right_ref[here, :] = pulled[:, half:]
        return (
            dgain + jnp.sum(by_gain, axis=0, keepdims=True),
            doffset + jnp.sum(grad, axis=0, keepdims=True),
        )

    none = jnp.zeros((1, features), f32)
    dgain, doffset = lax.fori_loop(0, left_ref.shape[0] // step, body, (none, none))
    sums_ref[...] = sums_in_ref[...]
    sums_ref[0:1, :] = dgain
    sums_ref[1:2, :] = doffset


def key_grad_kernel(compact_ref, factor_ref, normed_ref, spread_ref, row_ref, col_ref, out_ref):
    features = factor_ref.shape[1]

    @pl.loop(0, features // 256)
    def _(i):
        factor = stack_heads(factor_ref[:, group_slice(i)])
        wide = dot_nn(spread_ref[...], compact_ref[i])
        wide = jnp.where(row_ref[...] == col_ref[...], wide, 0.0).astype(bf16)
        joined = dot_nn(wide, factor).astype(bf16)
        out_ref[group_slice(i), :] = dot_tn(joined, normed_ref[...])


def owner_kernel(info_ref, a_ref, b0_ref, b1_ref, out_ref, square_ref):
    first = dot_tn(a_ref[...], b0_ref[0])
    second = dot_tn(a_ref[...], b1_ref[0])
    rows = lax.broadcasted_iota(jnp.int32, first.shape, 0)
    grad = jnp.where(rows < info_ref[2], first, second)
    place = rows + info_ref[3]
    grad = jnp.where((place < info_ref[4]) | (place >= info_ref[5]), grad, 0.0)
    out_ref[...] = grad
    square_ref[...] = jnp.sum(grad * grad, axis=0, keepdims=True)


def bits_of(axis):
    size = lax.axis_size(axis)
    return [1 << b for b in range(size.bit_length() - 1)]


def swapped(block, axis, bit):
    return lax.ppermute(block, axis, [(i, i ^ bit) for i in range(lax.axis_size(axis))])


def gathered(block, axis):
    for bit in reversed(bits_of(axis)):
        block = jnp.concatenate([block, swapped(block, axis, bit)], axis=0)
    return block


def place_in_gathered(device, axis):
    other = lax.axis_index(axis) ^ device
    order = list(reversed(bits_of(axis)))
    return sum(((other & bit) // bit) << s for s, bit in enumerate(order))


def summed_slice(block, axis):
    index = lax.axis_index(axis)
    for bit in bits_of(axis):
        half = block.shape[0] // 2
        upper = (index & bit) != 0
        sent = jnp.where(upper, block[:half], block[half:])
        kept = jnp.where(upper, block[half:], block[:half])
        block = kept + swapped(sent, axis, bit)
    return block


def share_of(index, size):
    bits = [1 << b for b in range(size.bit_length() - 1)]
    return sum(((index & bit) // bit) << (len(bits) - 1 - s) for s, bit in enumerate(bits))


def summed(block):
    for axis in ("dp", "tower"):
        for bit in bits_of(axis):
            block = block + swapped(block, axis, bit)
    return block


def local(
    images,
    captions,
    token_ids,
    counts,
    matches,
    image_weights,
    image_norms,
    weights,
    norm_params,
    momentum,
    norm_momentum,
    averages,
    norm_averages,
):
    text = lax.axis_index("tower") == 1
    index = lax.axis_index("dp")
    n = lax.axis_size("dp")
    both = ("tower", "dp")
    caps, length, features = captions.shape
    imgs, img_rows = images.shape[:2]
    text_rows = caps * length
    own_rows = weights.shape[0]
    all_rows = 2 * n * own_rows
    hidden_units = (all_rows - 4 * features) // 2
    count = round_up(max(caps, imgs), 8)
    total = round_up(max(text_rows, imgs * img_rows), 48)
    wide = GROUP * count

    low_shard = weights.astype(bf16)
    even = lax.ppermute(low_shard, both, [(2 * k, n + k) for k in range(n)])
    odd = lax.ppermute(low_shard, both, [(2 * k + 1, n + k) for k in range(n)])
    shard = jnp.where(text, jnp.concatenate([even, odd], axis=0), image_weights)
    packed = lax.all_gather(shard, "dp", axis=0, tiled=True)

    def padded(rows):
        return jnp.pad(rows.reshape(-1, features), ((0, total - rows.shape[0] * rows.shape[1]), (0, 0)))

    caption_x = padded(captions)
    lengths = jnp.sum((token_ids != 0).astype(jnp.int32), axis=1)
    start_t = jnp.arange(caps, dtype=jnp.int32) * length
    start_i = jnp.arange(imgs, dtype=jnp.int32) * img_rows

    def column(values, fill):
        return jnp.pad(values, (0, count - values.shape[0]), constant_values=fill)[:, None]

    low_t, high_t, pos_t = column(start_t, 0), column(start_t + lengths, 1), column(start_t + lengths - 1, 0)
    low_i, high_i, pos_i = column(start_i, 0), column(start_i + img_rows, 1), column(start_i, 0)
    rows_out = (
        sds((total, features), bf16),
        sds((count, features), bf16),
        sds((count, features), f32),
    )
    normed_t, npool_t, xpool_t = call(
        partial(rows_kernel, 48), rows_out, caption_x, pos_t, norm_params, name="rows"
    )
    normed_i, npool_i, xpool_i = call(
        partial(rows_kernel, 48), rows_out, padded(images), pos_i, image_norms, name="rows"
    )

    def mine(of_text, of_image):
        return jnp.where(text, of_text, of_image)

    normed, npool, xpool = mine(normed_t, normed_i), mine(npool_t, npool_i), mine(xpool_t, xpool_i)
    norms = mine(norm_params, image_norms)

    queries, key_rows, values, probs, attended, hidden, normed_mid = call(
        attend_kernel,
        (
            sds((count, features), bf16),
            sds((total, features), bf16),
            sds((total, features), bf16),
            sds((features // 256, wide, total), f32),
            sds((count, features), bf16),
            sds((count, features), f32),
            sds((count, features), bf16),
        ),
        normed, npool, xpool, norms, mine(low_t, low_i), mine(high_t, high_i),
        packed[: 4 * features],
        name="attend",
    )
    block = hidden_units // 8
    up_at, down_at = 4 * features // block, (4 * features + hidden_units) // block
    fixed = pl.BlockSpec((count, features), lambda i: (0, 0))
    up_spec = pl.BlockSpec((block, features), lambda i: (up_at + i, 0))
    down_spec = pl.BlockSpec((block, features), lambda i: (down_at + i, 0))
    slab = pl.BlockSpec((count, block), lambda i: (0, i))
    pre_act, activated, pooled, inverse, emb = pl.pallas_call(
        feed_kernel,
        grid=(8,),
        in_specs=[fixed, fixed, up_spec, down_spec],
        out_specs=(slab, slab, fixed, pl.BlockSpec((count, 128), lambda i: (0, 0)), fixed),
        out_shape=(
            sds((count, hidden_units), f32),
            sds((count, hidden_units), bf16),
            sds((count, features), f32),
            sds((count, 128), f32),
            sds((count, features), bf16),
        ),
        scratch_shapes=[pltpu.VMEM((count, features), f32)],
        name="feed",
    )(normed_mid, hidden, packed, packed)

    img_slots = round_up(imgs + 1, 8)
    count_row = jnp.pad(counts.astype(bf16), (0, features - imgs))[None]
    image_block = jnp.concatenate(
        [emb[:imgs], count_row, jnp.zeros((img_slots - imgs - 1, features), bf16)], axis=0
    )
    crossed = lax.ppermute(image_block, "tower", [(0, 1)])
    all_text = gathered(emb, "dp")
    all_images = gathered(crossed, "dp")
    owner_place = place_in_gathered(matches // imgs, "dp")
    place = column(owner_place * img_slots + matches % imgs, 0)
    count_place = column(owner_place * img_slots + imgs, 0)
    slot = column(matches % imgs, 0)
    real = (np.arange(count) < caps).astype(np.float32)[:, None]
    row_bias = np.tile(np.where(np.arange(count) < caps, 0.0, MASKED), n)[:, None]
    col_bias = np.tile(np.where(np.arange(img_slots) < imgs, 0.0, MASKED), n)[None]
    chunk = count * min(8, n)
    grad_rows, grad_branch = call(
        partial(loss_kernel, chunk, imgs),
        (sds((count, features), f32), sds((count, features), bf16)),
        all_text, all_images, jnp.asarray(row_bias, f32), jnp.asarray(col_bias, f32),
        emb, pooled, inverse, place, count_place, slot, jnp.asarray(real),
        name="loss",
    )

    grad_pre, grad_hidden, grad_mixed, sums = pl.pallas_call(
        feed_back_kernel,
        grid=(8,),
        in_specs=[
            fixed, fixed, fixed, pl.BlockSpec((4, features), lambda i: (0, 0)), slab,
            up_spec, down_spec,
        ],
        out_specs=(slab, fixed, fixed, pl.BlockSpec((8, features), lambda i: (0, 0))),
        out_shape=(
            sds((count, hidden_units), bf16),
            sds((count, features), f32),
            sds((count, features), bf16),
            sds((8, features), f32),
        ),
        scratch_shapes=[pltpu.VMEM((count, features), f32)],
        name="feed_back",
    )(grad_branch, grad_rows, hidden, norms, pre_act, packed, packed)
    half = features // 2
    groups = features // 256
    fold = (np.arange(total)[:, None] % length == np.arange(length)[None]).astype(np.float32)
    fold = jnp.asarray(fold, bf16)
    grad_att, grad_q, compact_raw, compact_prob, left, right, sums = call(
        partial(attend_back_kernel, 48, half),
        (
            sds((count, features), bf16),
            sds((count, features), bf16),
            sds((groups, length, wide), bf16),
            sds((groups, length, wide), bf16),
            sds((text_rows, half), bf16),
            sds((text_rows, features - half), f32),
            sds((8, features), f32),
        ),
        grad_mixed, grad_hidden, probs, queries, key_rows, values, caption_x,
        pos_t.reshape(1, count), norms, sums, fold, packed[: 4 * features],
        scratch=[pltpu.VMEM((total, features), f32)],
        name="attend_back",
    )

    lower = all_rows // 2 - 4 * features
    to_image = [(1, 0)]
    early = lax.ppermute(
        jnp.concatenate([queries, attended, normed_mid], axis=1), "tower", to_image
    )
    raw_x = lax.ppermute(compact_raw, "tower", to_image)
    late = lax.ppermute(
        jnp.concatenate([grad_q, grad_mixed, grad_pre[:, :lower]], axis=1), "tower", to_image
    )
    left_x = lax.ppermute(left, "tower", to_image)
    queries_x, attended_x = early[:, :features], early[:, features : 2 * features]
    mid_x = early[:, 2 * features :]
    columns = mine(
        jnp.concatenate([grad_pre[:, lower:], activated], axis=1),
        jnp.concatenate(
            [late[:, :features], jnp.zeros((count, 2 * features), bf16), late[:, features:]], axis=1
        ),
    )
    spread = columns.reshape(count, n, own_rows).transpose(1, 0, 2)
    own_columns = lax.all_to_all(spread, "dp", 0, 0, tiled=True).reshape(n * count, own_rows)
    others = jnp.stack(
        [mine(grad_branch, npool_t), mine(grad_branch, attended_x), mine(normed_mid, mid_x)]
    )
    others = lax.all_gather(others, "dp", axis=1, tiled=True)

    row_cap = jnp.asarray(np.arange(total)[:, None] // length, jnp.int32)
    col_cap = jnp.asarray(np.tile(np.arange(count), GROUP)[None], jnp.int32)
    kv_part = call(
        key_grad_kernel,
        sds((features, features), f32),
        mine(compact_prob, raw_x), mine(grad_att, queries_x), normed_t, fold, row_cap, col_cap,
        name="key_grad",
    )
    kv_share = summed_slice(kv_part, "dp")
    share_rows = features // n
    slots = own_rows // share_rows
    holder = {share_of(i, n): i for i in range(n)}
    placed = []
    for s in range(slots):
        route = []
        for owner in range(2 * n):
            row = owner * own_rows + s * share_rows
            if features <= row < 3 * features:
                tower, at = divmod((row - features) // share_rows, n)
                route.append((tower * n + holder[at], owner))
        placed.append(lax.ppermute(kv_share, both, route))
    kv_rows = jnp.concatenate(placed, axis=0)

    first_row = (lax.axis_index("tower") * n + index) * own_rows
    last_row = first_row + own_rows - 1
    up_row, down_row = 4 * features, 4 * features + hidden_units

    def other_of(row):
        in_low = jnp.where(row < 3 * features, 0, jnp.where(row < up_row, 1, 2))
        return jnp.where(row >= down_row, 0, in_low)

    edges = jnp.array([features, 3 * features, up_row, down_row], jnp.int32)
    inside = (edges > first_row) & (edges <= last_row)
    edge = jnp.min(jnp.where(inside, edges - first_row, own_rows))
    info = jnp.stack(
        [
            other_of(first_row), other_of(last_row), edge, first_row,
            jnp.int32(features), jnp.int32(3 * features),
        ]
    ).astype(jnp.int32)
    own_grads, squares = pl.pallas_call(
        owner_kernel,
        grid_spec=pltpu.PrefetchScalarGridSpec(
            num_scalar_prefetch=1,
            grid=(1,),
            in_specs=[
                pl.BlockSpec((n * count, own_rows), lambda i, s: (0, 0)),
                pl.BlockSpec((1, n * count, features), lambda i, s: (s[0], 0, 0)),
                pl.BlockSpec((1, n * count, features), lambda i, s: (s[1], 0, 0)),
            ],
            out_specs=(
                pl.BlockSpec((own_rows, features), lambda i, s: (0, 0)),
                pl.BlockSpec((1, features), lambda i, s: (0, 0)),
            ),
        ),
        out_shape=(sds((own_rows, features), f32), sds((1, features), f32)),
        name="owner",
    )(info, own_columns, others, others)

    squares = squares + jnp.sum(kv_share * kv_share, axis=0, keepdims=True)
    sums = jnp.where(text, sums, 0.0)
    sums = summed(jnp.concatenate([sums[:4], squares, sums[5:]], axis=0))
    total_norm_grads = sums[:4]
    grad_norm = jnp.sqrt(jnp.sum(sums[4]) + jnp.sum(total_norm_grads * total_norm_grads))
    factor = jnp.minimum(1.0, CLIP_NORM / (grad_norm + 1e-06))
    grads = (own_grads + kv_rows) * factor
    norm_grads = total_norm_grads * factor
    step_rate = 0.4 * math.sqrt(all_rows)
    decayed = grads + DECAY_RATE * weights
    new_momentum = MOMENTUM_RATE * momentum + decayed
    new_weights = weights - step_rate * (decayed + MOMENTUM_RATE * new_momentum)
    new_averages = AVERAGE_RATE * averages + (1.0 - AVERAGE_RATE) * new_weights
    new_norm_momentum = MOMENTUM_RATE * norm_momentum + norm_grads
    new_norm_params = norm_params - step_rate * (norm_grads + MOMENTUM_RATE * new_norm_momentum)
    new_norm_averages = AVERAGE_RATE * norm_averages + (1.0 - AVERAGE_RATE) * new_norm_params
    input_grad = jnp.where(text, right, left_x.astype(f32)).reshape(caps, length, half)
    return (
        grads,
        norm_grads,
        input_grad,
        new_weights,
        new_momentum,
        new_averages,
        new_norm_params,
        new_norm_momentum,
        new_norm_averages,
        grad_norm,
    )


def solution(mesh):
    return jax.shard_map(
        local,
        mesh=mesh,
        in_specs=(
            P("dp", None, None),
            P("dp", None, None),
            P("dp", None),
            P("dp"),
            P("dp"),
            P("dp", None),
            P(),
            P(("tower", "dp"), None),
            P(),
            P(("tower", "dp"), None),
            P(),
            P(("tower", "dp"), None),
            P(),
        ),
        out_specs=(
            P(("tower", "dp"), None),
            P(),
            P("dp", None, "tower"),
            P(("tower", "dp"), None),
            P(("tower", "dp"), None),
            P(("tower", "dp"), None),
            P(),
            P(),
            P(),
            P(),
        ),
        check_vma=False,
    )
```

```python
from functools import partial
import math

import jax
import jax.numpy as jnp
import numpy as np
from jax import lax
from jax.experimental import pallas as pl
from jax.experimental.pallas import tpu as pltpu
from jax.sharding import PartitionSpec as P

HEAD_DIM = 64
GROUP = 4

EPSILON = 1e-06
LOGIT_SCALE = 50.0
CLIP_NORM = 1.0
MOMENTUM_RATE = 0.9
DECAY_RATE = 0.0001
AVERAGE_RATE = 0.7
MASKED = -1e30
GELU_A = 0.044715
GELU_C = math.sqrt(2.0 / math.pi)

POS_TEXT, POS_IMAGE, LOW, HIGH, PLACE, COUNT_PLACE, SLOT, REAL = range(8)

f32 = jnp.float32
bf16 = jnp.bfloat16


def round_up(value, step):
    return (value + step - 1) // step * step


def dot_nn(left, right, **kw):
    return lax.dot_general(
        left, right, (((1,), (0,)), ((), ())), preferred_element_type=f32, **kw
    )


def dot_nt(left, right):
    return lax.dot_general(left, right, (((1,), (1,)), ((), ())), preferred_element_type=f32)


def dot_tn(left, right):
    return lax.dot_general(left, right, (((0,), (0,)), ((), ())), preferred_element_type=f32)


def call(kernel, outs, *args, scratch=(), name=None, weights=None, smem=None):
    whole = pl.BlockSpec(memory_space=pltpu.VMEM)
    specs = [whole] * len(args)
    if smem is not None:
        specs = [pl.BlockSpec(memory_space=pltpu.SMEM)] + specs
        args = (smem, *args)
    if weights is not None:
        parts, table = weights
        specs = (
            [pl.BlockSpec(memory_space=pltpu.SMEM)]
            + [pl.BlockSpec(memory_space=pltpu.HBM)] * len(parts)
            + specs
        )
        args = (table, *parts, *args)
    return pl.pallas_call(
        kernel,
        out_shape=outs,
        in_specs=specs,
        out_specs=jax.tree.map(lambda _: whole, outs),
        scratch_shapes=list(scratch),
        name=name,
    )(*args)


def sds(shape, dtype):
    return jax.ShapeDtypeStruct(shape, dtype)


def normalize(rows):
    middle = jnp.mean(rows, axis=-1, keepdims=True)
    centred = rows - middle
    spread = jnp.mean(centred * centred, axis=-1, keepdims=True)
    scale = lax.rsqrt(spread + EPSILON)
    return centred * scale, scale


def norm_pull(grad, rows, gain):
    unit, scale = normalize(rows)
    scaled = grad * gain
    pulled = scale * (
        scaled
        - jnp.mean(scaled, axis=-1, keepdims=True)
        - unit * jnp.mean(scaled * unit, axis=-1, keepdims=True)
    )
    return pulled, grad * unit


def lanes_of_heads(count):
    return lax.broadcasted_iota(jnp.int32, (count, GROUP * HEAD_DIM), 1) // HEAD_DIM


def stack_heads(block):
    lanes = lanes_of_heads(block.shape[0])
    zero = jnp.zeros_like(block)
    return jnp.concatenate([jnp.where(lanes == h, block, zero) for h in range(GROUP)], axis=0)


def unstack_heads(block):
    count = block.shape[0] // GROUP
    lanes = lanes_of_heads(count)
    total = jnp.where(lanes == 0, block[:count], 0.0)
    for h in range(1, GROUP):
        total = jnp.where(lanes == h, block[h * count : (h + 1) * count], total)
    return total


def group_slice(index, base=0):
    return pl.ds(pl.multiple_of(base + index * 256, 256), 256)


def rows_kernel(
    step, text_ref, captions_ref, images_ref, facts_ref, norms_t_ref, norms_i_ref,
    normed_t_ref, normed_ref, npool_t_ref, npool_ref, xpool_ref, facts_out_ref, norms_ref,
):
    facts_out_ref[...] = facts_ref[...]
    norms_ref[...] = jnp.where(text_ref[0] == 1, norms_t_ref[...], norms_i_ref[...])

    def pooled(x_ref, fact, from_ref, to_ref):
        count = to_ref.shape[0]
        pick = (
            lax.broadcasted_iota(jnp.int32, (count, x_ref.shape[0]), 1)
            == facts_ref[:, fact : fact + 1]
        ).astype(bf16)
        to_ref[...] = dot_nn(pick, from_ref[...]).astype(bf16)
        xpool_ref[...] = dot_nn(pick, x_ref[...])

    @pl.loop(0, captions_ref.shape[0] // step)
    def _(i):
        here = pl.ds(pl.multiple_of(i * step, step), step)
        unit, _ = normalize(captions_ref[here, :].astype(f32))
        normed_t_ref[here, :] = (unit * norms_t_ref[0:1, :] + norms_t_ref[1:2, :]).astype(bf16)

    pooled(captions_ref, POS_TEXT, normed_t_ref, npool_t_ref)

    @pl.when(text_ref[0] == 1)
    def _():
        normed_ref[...] = normed_t_ref[...]
        npool_ref[...] = npool_t_ref[...]

    @pl.when(text_ref[0] == 0)
    def _():
        @pl.loop(0, images_ref.shape[0] // step)
        def _(i):
            here = pl.ds(pl.multiple_of(i * step, step), step)
            unit, _ = normalize(images_ref[here, :].astype(f32))
            normed_ref[here, :] = (unit * norms_i_ref[0:1, :] + norms_i_ref[1:2, :]).astype(bf16)

        pooled(images_ref, POS_IMAGE, normed_ref, npool_ref)


def attend_kernel(parts, table_ref, *refs):
    part_refs = refs[:parts]
    (
        normed_ref, npool_ref, xpool_ref, norms_ref, facts_ref,
        q_ref, k_ref, v_ref, probs_ref, att_ref, hidden_ref, nm_ref, w_ref, sems,
    ) = refs[parts:]
    count, features = npool_ref.shape
    for wait in fetch(table_ref, part_refs, 0, 4 * features, w_ref, sems):
        wait()
    total = normed_ref.shape[0]
    keys = lax.broadcasted_iota(jnp.int32, (count, total), 1)
    allowed = ((keys >= facts_ref[:, LOW : LOW + 1]) & (keys < facts_ref[:, HIGH : HIGH + 1]))[None]

    @pl.loop(0, features // 256)
    def _(i):
        cols = group_slice(i)
        queries = dot_nt(npool_ref[...], w_ref[group_slice(i), :]).astype(bf16)
        key_rows = dot_nt(normed_ref[...], w_ref[group_slice(i, features), :]).astype(bf16)
        values = dot_nt(normed_ref[...], w_ref[group_slice(i, 2 * features), :]).astype(bf16)
        q_ref[:, cols] = queries
        k_ref[:, cols] = key_rows
        v_ref[:, cols] = values
        scores = dot_nt(stack_heads(queries), key_rows) * HEAD_DIM**-0.5
        scores = jnp.where(allowed, scores.reshape(GROUP, count, total), MASKED)
        exponent = jnp.exp(scores - jnp.max(scores, axis=-1, keepdims=True))
        probs = exponent / jnp.sum(exponent, axis=-1, keepdims=True)
        probs = probs.reshape(GROUP * count, total)
        probs_ref[i] = probs
        att_ref[:, cols] = unstack_heads(dot_nn(probs.astype(bf16), values)).astype(bf16)

    hidden = xpool_ref[...] + dot_nt(
        att_ref[...], w_ref[pl.ds(3 * features, features), :]
    )
    hidden_ref[...] = hidden
    unit, _ = normalize(hidden)
    nm_ref[...] = (unit * norms_ref[2:3, :] + norms_ref[3:4, :]).astype(bf16)


def gelu_parts(pre):
    tanh = jnp.tanh(GELU_C * (pre + GELU_A * pre * pre * pre))
    return 0.5 * (1.0 + tanh), tanh


def feed_kernel(parts, first, skip, block, table_ref, *refs):
    part_refs = refs[:parts]
    (
        nm_ref, hidden_ref, pre_ref, act_ref, pooled_ref, inverse_ref, emb_ref, w_ref, total_ref, sems,
    ) = refs[parts:]
    units = pre_ref.shape[1]
    for wait in fetch(table_ref, part_refs, first, w_ref.shape[0], w_ref, sems):
        wait()
    total_ref[...] = hidden_ref[...]

    @pl.loop(0, units // block)
    def _(i):
        here = pl.ds(pl.multiple_of(i * block, block), block)
        pre = dot_nt(nm_ref[...], w_ref[pl.ds(pl.multiple_of(skip + i * block, 64), block), :])
        pre_ref[:, here] = pre
        act = (pre * gelu_parts(pre)[0]).astype(bf16)
        act_ref[:, here] = act
        total_ref[...] += dot_nn(
            act, w_ref[pl.ds(pl.multiple_of(skip + units + i * block, 64), block), :]
        )

    pooled = total_ref[...]
    inverse = lax.rsqrt(jnp.sum(pooled * pooled, axis=-1, keepdims=True) + EPSILON)
    pooled_ref[...] = pooled
    inverse_ref[...] = jnp.broadcast_to(inverse, inverse_ref.shape)
    emb_ref[...] = (pooled * inverse).astype(bf16)


def loss_kernel(
    chunk, slots, text_ref, img_ref, row_bias_ref, col_bias_ref, emb_ref, pooled_ref, inverse_ref,
    facts_ref, grad_ref, branch_ref,
):
    images = img_ref.shape[0]
    count = emb_ref.shape[0]

    def body(j, carry):
        top, acc = carry
        here = pl.ds(pl.multiple_of(j * chunk, chunk), chunk)
        logits = LOGIT_SCALE * dot_nt(text_ref[here, :], img_ref[...]) + row_bias_ref[here, :]
        higher = jnp.maximum(top, jnp.max(logits, axis=0, keepdims=True))
        acc = acc * jnp.exp(top - higher) + jnp.sum(
            jnp.exp(logits - higher), axis=0, keepdims=True
        )
        return higher, acc

    top, acc = lax.fori_loop(
        0,
        text_ref.shape[0] // chunk,
        body,
        (jnp.full((1, images), MASKED, f32), jnp.zeros((1, images), f32)),
    )
    column_lse = top + jnp.log(acc)
    logits = LOGIT_SCALE * dot_nt(emb_ref[...], img_ref[...])
    masked = logits + col_bias_ref[...]
    row_top = jnp.max(masked, axis=1, keepdims=True)
    row_exp = jnp.exp(masked - row_top)
    by_row = row_exp / jnp.sum(row_exp, axis=1, keepdims=True)
    by_column = jnp.exp(masked - column_lse)
    columns = lax.broadcasted_iota(jnp.int32, (count, images), 1)
    target = (columns == facts_ref[:, PLACE : PLACE + 1]).astype(f32)
    listed = dot_nn((columns == facts_ref[:, COUNT_PLACE : COUNT_PLACE + 1]).astype(bf16), img_ref[...])
    at = lax.broadcasted_iota(jnp.int32, listed.shape, 1) == facts_ref[:, SLOT : SLOT + 1]
    named = jnp.maximum(jnp.sum(jnp.where(at, listed, 0.0), axis=1, keepdims=True), 1.0)
    grad_logits = 0.5 * (by_row - target) + 0.5 * (by_column - target / named)
    scaled = jnp.where(
        (col_bias_ref[...] == 0.0) & (facts_ref[:, REAL : REAL + 1] > 0), LOGIT_SCALE * grad_logits, 0.0
    ).astype(bf16)
    grad_embed = dot_nn(scaled, img_ref[...])
    pooled = pooled_ref[...]
    inverse = inverse_ref[:, 0:1]
    projection = jnp.sum(pooled * grad_embed, axis=-1, keepdims=True)
    grad_pooled = inverse * grad_embed - inverse * inverse * inverse * projection * pooled
    grad_ref[...] = grad_pooled
    branch_ref[...] = grad_pooled.astype(bf16)


def feed_back_kernel(parts, first, skip, block, table_ref, *refs):
    part_refs = refs[:parts]
    (
        branch_ref, grad_ref, hidden_ref, norms_ref, pre_ref,
        gpre_ref, ghidden_ref, mixed_ref, sums_ref, gatt_ref, w_ref, total_ref, sems,
    ) = refs[parts:]
    units = pre_ref.shape[1]
    features = branch_ref.shape[1]
    for wait in fetch(table_ref, part_refs, first, w_ref.shape[0], w_ref, sems):
        wait()
    total_ref[...] = jnp.zeros_like(total_ref)

    @pl.loop(0, units // block)
    def _(i):
        here = pl.ds(pl.multiple_of(i * block, block), block)
        pre = pre_ref[:, here]
        cdf, tanh = gelu_parts(pre)
        slope = cdf + pre * 0.5 * (1.0 - tanh * tanh) * GELU_C * (1.0 + 3.0 * GELU_A * pre * pre)
        grad_act = dot_nt(
            branch_ref[...], w_ref[pl.ds(pl.multiple_of(skip + units + i * block, 64), block), :]
        ).astype(bf16)
        gpre = (grad_act.astype(f32) * slope).astype(bf16)
        gpre_ref[:, here] = gpre
        total_ref[...] += dot_nn(gpre, w_ref[pl.ds(pl.multiple_of(skip + i * block, 64), block), :])

    grad = total_ref[...]
    pulled, by_gain = norm_pull(grad, hidden_ref[...], norms_ref[2:3, :])
    ghidden = grad_ref[...] + pulled
    mixed = ghidden.astype(bf16)
    ghidden_ref[...] = ghidden
    mixed_ref[...] = mixed
    gatt_ref[...] = dot_nn(mixed, w_ref[pl.ds(skip - features, features), :]).astype(bf16)
    sums_ref[...] = jnp.zeros_like(sums_ref)
    sums_ref[2:3, :] = jnp.sum(by_gain, axis=0, keepdims=True)
    sums_ref[3:4, :] = jnp.sum(grad, axis=0, keepdims=True)


def attend_back_kernel(parts, step, half, table_ref, *refs):
    part_refs = refs[:parts]
    (
        gatt_ref, ghidden_ref, probs_ref, q_ref, k_ref, v_ref, x_ref, facts_ref, norms_ref,
        sums_in_ref, fold_ref,
        gq_ref, craw_ref, cprob_ref, left_ref, right_ref, sums_ref, grad_ref, w_ref, sems,
    ) = refs[parts:]
    count, features = gatt_ref.shape
    for wait in fetch(table_ref, part_refs, 0, 3 * features, w_ref, sems):
        wait()

    @pl.loop(0, features // 256)
    def _(i):
        cols = group_slice(i)
        gatt = stack_heads(gatt_ref[:, cols])
        queries = stack_heads(q_ref[:, cols])
        key_rows, values = k_ref[:, cols], v_ref[:, cols]
        probs = probs_ref[i]
        grad_probs = dot_nt(gatt, values)
        mean = jnp.sum(probs * grad_probs, axis=-1, keepdims=True)
        raw = (probs * (grad_probs - mean) * HEAD_DIM**-0.5).astype(bf16)
        low = probs.astype(bf16)
        gq_ref[:, cols] = unstack_heads(dot_nn(raw, key_rows)).astype(bf16)
        gk = dot_tn(raw, queries).astype(bf16)
        gv = dot_tn(low, gatt).astype(bf16)
        part = dot_nn(gk, w_ref[group_slice(i, features), :]) + dot_nn(
            gv, w_ref[group_slice(i, 2 * features), :]
        )

        @pl.when(i == 0)
        def _():
            grad_ref[...] = part

        @pl.when(i > 0)
        def _():
            grad_ref[...] += part

        fold = fold_ref[...]
        craw_ref[i] = lax.dot_general(
            fold, raw, (((0,), (1,)), ((), ())), preferred_element_type=f32
        ).astype(bf16)
        cprob_ref[i] = lax.dot_general(
            fold, low, (((0,), (1,)), ((), ())), preferred_element_type=f32
        ).astype(bf16)

    gpool = dot_nn(gq_ref[...], w_ref[pl.ds(0, features), :])
    gain = norms_ref[0:1, :]

    def body(j, carry):
        dgain, doffset = carry
        here = pl.ds(pl.multiple_of(j * step, step), step)
        pick = (
            lax.broadcasted_iota(jnp.int32, (step, count), 0) + j * step
            == facts_ref[POS_TEXT : POS_TEXT + 1, :]
        ).astype(f32)
        grad = grad_ref[here, :] + dot_nn(pick, gpool, precision=lax.Precision.HIGHEST)
        pulled, by_gain = norm_pull(grad, x_ref[here, :].astype(f32), gain)
        pulled = pulled + dot_nn(pick, ghidden_ref[...], precision=lax.Precision.HIGHEST)
        left_ref[here, :] = pulled[:, :half].astype(bf16)
        right_ref[here, :] = pulled[:, half:]
        return (
            dgain + jnp.sum(by_gain, axis=0, keepdims=True),
            doffset + jnp.sum(grad, axis=0, keepdims=True),
        )

    none = jnp.zeros((1, features), f32)
    dgain, doffset = lax.fori_loop(0, left_ref.shape[0] // step, body, (none, none))
    sums_ref[...] = sums_in_ref[...]
    sums_ref[0:1, :] = dgain
    sums_ref[1:2, :] = doffset


def key_grad_kernel(compact_ref, factor_ref, normed_ref, spread_ref, row_ref, col_ref, out_ref):
    features = factor_ref.shape[1]

    @pl.loop(0, features // 256)
    def _(i):
        factor = stack_heads(factor_ref[:, group_slice(i)])
        wide = dot_nn(spread_ref[...], compact_ref[i])
        wide = jnp.where(row_ref[...] == col_ref[...], wide, 0.0).astype(bf16)
        joined = dot_nn(wide, factor).astype(bf16)
        out_ref[group_slice(i), :] = dot_tn(joined, normed_ref[...])


def owner_kernel(info_ref, a_ref, b0_ref, b1_ref, out_ref, square_ref):
    first = dot_tn(a_ref[...], b0_ref[0])
    second = dot_tn(a_ref[...], b1_ref[0])
    rows = lax.broadcasted_iota(jnp.int32, first.shape, 0)
    grad = jnp.where(rows < info_ref[2], first, second)
    place = rows + info_ref[3]
    grad = jnp.where((place < info_ref[4]) | (place >= info_ref[5]), grad, 0.0)
    out_ref[...] = grad
    square_ref[...] = jnp.sum(grad * grad, axis=0, keepdims=True)


def bits_of(axis):
    size = lax.axis_size(axis)
    return [1 << b for b in range(size.bit_length() - 1)]


def swapped(block, axis, bit):
    return lax.ppermute(block, axis, [(i, i ^ bit) for i in range(lax.axis_size(axis))])


UNITS = 16


def units_gathered(low_shard, image_weights, text, prepare):
    n = lax.axis_size("dp")
    chips = n // 2
    steps = chips // 2
    index = lax.axis_index("dp")
    core = index % 2
    other_core = [(i, i ^ 1) for i in range(n)]
    order = list(range(0, chips, 2)) + list(range(1, chips, 2))[::-1]
    seat_of = np.zeros(chips, np.int32)
    seat_of[order] = np.arange(chips)
    route = []
    for s in range(chips):
        route.append((2 * order[s], 2 * order[(s + 1) % chips]))
        route.append((2 * order[s] + 1, 2 * order[s - 1] + 1))

    def pair(own, other):
        return jnp.where(
            core == 0,
            jnp.concatenate([own, other], axis=0),
            jnp.concatenate([other, own], axis=0),
        )

    def swap(block):
        return lax.ppermute(block, "dp", other_core)

    def onward(block):
        return lax.ppermute(block, "dp", route)

    def half_of(block):
        size = block.shape[0] // 2
        return lax.dynamic_slice_in_dim(block, core * size, size, axis=0)

    high = swap(low_shard)
    image = swap(image_weights)
    b_part = jnp.where(text, pair(low_shard, high), jnp.where(core == 0, image, image_weights))
    low_shard, image, image_weights, b_part = lax.optimization_barrier(
        (low_shard, image, image_weights, b_part)
    )
    over = lax.ppermute(low_shard, "tower", [(0, 1)])
    low = swap(over)
    a_part = jnp.where(text, pair(over, low), jnp.where(core == 0, image_weights, image))

    unit = np.arange(UNITS)
    part = jnp.where(text, unit // chips, unit % 2)
    far = (seat_of[None] - seat_of[:, None]) % chips
    own_far = jnp.sum(
        jnp.where(jnp.arange(chips)[None] == index // 2, jnp.asarray(far), 0), axis=1
    )
    far = jnp.where(text, jnp.tile(own_far, 2), jnp.repeat(own_far, 2))
    step = jnp.minimum(far, chips - far)
    from_other = (far < steps) == (core == 1)
    table = jnp.where(
        far == 0,
        part,
        jnp.where(
            far == steps,
            4 * steps - 2 + 2 * part + core,
            4 * step - 2 + part + 2 * from_other,
        ),
    ).astype(jnp.int32)

    parts = [a_part, b_part]
    sent_a, sent_b = a_part, b_part
    prepared = prepare(b_part)
    for step in range(1, steps):
        sent_b = onward(sent_b)
        if step == 1:
            sent_a, sent_b = lax.optimization_barrier((sent_a, sent_b))
        elif step == 2:
            sent_a, prepared, table = lax.optimization_barrier((sent_a, prepared, table))
        sent_a = onward(sent_a)
        parts += [sent_a, sent_b, swap(sent_a), swap(sent_b)]
    last_b = onward(half_of(sent_b))
    last_a = onward(half_of(sent_a))
    parts += [last_a, swap(last_a), last_b, swap(last_b)]
    return parts, table, prepared


def fetch(table_ref, part_refs, first, rows, to_ref, sems):
    size = part_refs[0].shape[0]
    half = size // 2
    whole = [p for p in part_refs if p.shape[0] == size]
    halves = part_refs[len(whole) :]
    waits = []
    for u in range(-(-rows // size)):
        taken = min(size, rows - u * size)

        def copy(from_ref, at, count, u=u):
            return pltpu.make_async_copy(
                from_ref.at[pl.ds(0, count), :], to_ref.at[pl.ds(u * size + at, count), :], sems.at[u]
            )

        for j, part_ref in enumerate(whole):

            @pl.when(table_ref[first + u] == j)
            def _(part_ref=part_ref):
                copy(part_ref, 0, taken).start()

        for j in range(len(halves)):

            @pl.when(table_ref[first + u] == len(whole) + j)
            def _(j=j):
                mine, other = halves[j // 2 * 2], halves[j // 2 * 2 + 1]
                upper, lower = (mine, other) if j % 2 == 0 else (other, mine)
                copy(upper, 0, min(half, taken)).start()
                if taken > half:
                    copy(lower, half, taken - half).start()

        waits.append(copy(whole[0], 0, taken).wait)
    return waits


def gathered(block, axis):
    for bit in reversed(bits_of(axis)):
        block = jnp.concatenate([block, swapped(block, axis, bit)], axis=0)
    return block


def place_in_gathered(device, axis):
    other = lax.axis_index(axis) ^ device
    order = list(reversed(bits_of(axis)))
    return sum(((other & bit) // bit) << s for s, bit in enumerate(order))


def summed_slice(block, axis):
    index = lax.axis_index(axis)
    for bit in bits_of(axis):
        half = block.shape[0] // 2
        upper = (index & bit) != 0
        sent = jnp.where(upper, block[:half], block[half:])
        kept = jnp.where(upper, block[half:], block[:half])
        block = kept + swapped(sent, axis, bit)
    return block


def share_of(index, size):
    bits = [1 << b for b in range(size.bit_length() - 1)]
    return sum(((index & bit) // bit) << (len(bits) - 1 - s) for s, bit in enumerate(bits))


def summed(block):
    for axis in ("dp", "tower"):
        for bit in bits_of(axis):
            block = block + swapped(block, axis, bit)
    return block


def local(
    images,
    captions,
    token_ids,
    counts,
    matches,
    image_weights,
    image_norms,
    weights,
    norm_params,
    momentum,
    norm_momentum,
    averages,
    norm_averages,
):
    text = lax.axis_index("tower") == 1
    index = lax.axis_index("dp")
    n = lax.axis_size("dp")
    both = ("tower", "dp")
    caps, length, features = captions.shape
    imgs, img_rows = images.shape[:2]
    text_rows = caps * length
    own_rows = weights.shape[0]
    all_rows = 2 * n * own_rows
    hidden_units = (all_rows - 4 * features) // 2
    count = round_up(max(caps, imgs), 8)
    total = round_up(max(text_rows, imgs * img_rows), 48)
    wide = GROUP * count

    def mine(of_text, of_image):
        return jnp.where(text, of_text, of_image)

    def padded_to(values, fill):
        return jnp.pad(values, (0, count - values.shape[0]), constant_values=fill)

    def padded(rows):
        return jnp.pad(rows.reshape(-1, features), ((0, total - rows.shape[0] * rows.shape[1]), (0, 0)))

    img_slots = round_up(imgs + 1, 8)

    def prepare(ready):
        caption_in, image_in, ids, named, tallies, _ = lax.optimization_barrier(
            (captions, images, token_ids, matches, counts, ready)
        )
        caption_x = padded(caption_in)
        lengths = jnp.sum((ids != 0).astype(jnp.int32), axis=1)
        start_t = jnp.arange(caps, dtype=jnp.int32) * length
        start_i = jnp.arange(imgs, dtype=jnp.int32) * img_rows
        pos_t = start_t + lengths - 1
        owner_place = place_in_gathered(named // imgs, "dp")
        columns = [
            padded_to(pos_t, 0),
            padded_to(start_i, 0),
            mine(padded_to(start_t, 0), padded_to(start_i, 0)),
            mine(padded_to(start_t + lengths, 1), padded_to(start_i + img_rows, 1)),
            padded_to(owner_place * img_slots + named % imgs, 0),
            padded_to(owner_place * img_slots + imgs, 0),
            padded_to(named % imgs, 0),
            jnp.asarray(np.arange(count) < caps, jnp.int32),
        ]
        facts = jnp.stack(columns, axis=0)
        table = jnp.pad(facts.T, ((0, 0), (0, 128 - len(columns))))
        rows = call(
            partial(rows_kernel, 48),
            (
                sds((total, features), bf16),
                sds((total, features), bf16),
                sds((count, features), bf16),
                sds((count, features), bf16),
                sds((count, features), f32),
                sds((count, 128), jnp.int32),
                sds((4, features), f32),
            ),
            caption_x, padded(image_in), table, norm_params, image_norms,
            smem=text.astype(jnp.int32)[None],
            name="rows",
        )
        count_row = jnp.pad(tallies.astype(bf16), (0, features - imgs))[None]
        return caption_x, facts, rows, count_row

    low_shard = weights.astype(bf16)
    if n == UNITS:
        parts, table, prepared = units_gathered(low_shard, image_weights, text, prepare)
    else:
        even = lax.ppermute(low_shard, both, [(2 * k, n + k) for k in range(n)])
        odd = lax.ppermute(low_shard, both, [(2 * k + 1, n + k) for k in range(n)])
        shard = jnp.where(text, jnp.concatenate([even, odd], axis=0), image_weights)
        packed = lax.all_gather(shard, "dp", axis=0, tiled=True)
        parts = jnp.split(packed, UNITS, axis=0)
        table = jnp.arange(UNITS, dtype=jnp.int32)
        prepared = prepare(shard)
    caption_x, facts, rows, count_row = prepared
    normed_t, normed, npool_t, npool, xpool, facts_by_row, norms = rows
    part_rows = all_rows // UNITS
    feed_part = 4 * features // part_rows
    feed_skip = 4 * features - feed_part * part_rows

    queries, key_rows, values, probs, attended, hidden, normed_mid = call(
        partial(attend_kernel, len(parts)),
        (
            sds((count, features), bf16),
            sds((total, features), bf16),
            sds((total, features), bf16),
            sds((features // 256, wide, total), f32),
            sds((count, features), bf16),
            sds((count, features), f32),
            sds((count, features), bf16),
        ),
        normed, npool, xpool, norms, facts_by_row,
        scratch=[
            pltpu.VMEM((4 * features, features), bf16),
            pltpu.SemaphoreType.DMA((-(-4 * features // part_rows),)),
        ],
        weights=(parts, table),
        name="attend",
    )
    feed_rows = 2 * hidden_units + feed_skip
    block = hidden_units // 8
    pre_act, activated, pooled, inverse, emb = call(
        partial(feed_kernel, len(parts), feed_part, feed_skip, block),
        (
            sds((count, hidden_units), f32),
            sds((count, hidden_units), bf16),
            sds((count, features), f32),
            sds((count, 128), f32),
            sds((count, features), bf16),
        ),
        normed_mid, hidden,
        scratch=[
            pltpu.VMEM((feed_rows, features), bf16),
            pltpu.VMEM((count, features), f32),
            pltpu.SemaphoreType.DMA((-(-feed_rows // part_rows),)),
        ],
        weights=(parts, table),
        name="feed",
    )

    image_block = jnp.concatenate(
        [emb[:imgs], count_row, jnp.zeros((img_slots - imgs - 1, features), bf16)], axis=0
    )
    crossed = lax.ppermute(image_block, "tower", [(0, 1)])
    all_text = gathered(emb, "dp")
    all_images = gathered(crossed, "dp")
    row_bias = np.tile(np.where(np.arange(count) < caps, 0.0, MASKED), n)[:, None]
    col_bias = np.tile(np.where(np.arange(img_slots) < imgs, 0.0, MASKED), n)[None]
    chunk = count * min(8, n)
    grad_rows, grad_branch = call(
        partial(loss_kernel, chunk, imgs),
        (sds((count, features), f32), sds((count, features), bf16)),
        all_text, all_images, jnp.asarray(row_bias, f32), jnp.asarray(col_bias, f32),
        emb, pooled, inverse, facts_by_row,
        name="loss",
    )

    back_part = 3 * features // part_rows
    back_skip = 4 * features - back_part * part_rows
    back_rows = 2 * hidden_units + back_skip
    grad_pre, grad_hidden, grad_mixed, sums, grad_att = call(
        partial(feed_back_kernel, len(parts), back_part, back_skip, block),
        (
            sds((count, hidden_units), bf16),
            sds((count, features), f32),
            sds((count, features), bf16),
            sds((8, features), f32),
            sds((count, features), bf16),
        ),
        grad_branch, grad_rows, hidden, norms, pre_act,
        scratch=[
            pltpu.VMEM((back_rows, features), bf16),
            pltpu.VMEM((count, features), f32),
            pltpu.SemaphoreType.DMA((-(-back_rows // part_rows),)),
        ],
        weights=(parts, table),
        name="feed_back",
    )
    half = features // 2
    groups = features // 256
    fold = (np.arange(total)[:, None] % length == np.arange(length)[None]).astype(np.float32)
    fold = jnp.asarray(fold, bf16)
    grad_q, compact_raw, compact_prob, left, right, sums = call(
        partial(attend_back_kernel, len(parts), 48, half),
        (
            sds((count, features), bf16),
            sds((groups, length, wide), bf16),
            sds((groups, length, wide), bf16),
            sds((text_rows, half), bf16),
            sds((text_rows, features - half), f32),
            sds((8, features), f32),
        ),
        grad_att, grad_hidden, probs, queries, key_rows, values, caption_x,
        facts, norms, sums, fold,
        scratch=[
            pltpu.VMEM((total, features), f32),
            pltpu.VMEM((3 * features, features), bf16),
            pltpu.SemaphoreType.DMA((-(-3 * features // part_rows),)),
        ],
        weights=(parts, table),
        name="attend_back",
    )

    lower = all_rows // 2 - 4 * features
    to_image = [(1, 0)]
    early = lax.ppermute(
        jnp.concatenate([queries, attended, normed_mid], axis=1), "tower", to_image
    )
    raw_x = lax.ppermute(compact_raw, "tower", to_image)
    late = lax.ppermute(
        jnp.concatenate([grad_q, grad_mixed, grad_pre[:, :lower]], axis=1), "tower", to_image
    )
    left_x = lax.ppermute(left, "tower", to_image)
    queries_x, attended_x = early[:, :features], early[:, features : 2 * features]
    mid_x = early[:, 2 * features :]
    columns = mine(
        jnp.concatenate([grad_pre[:, lower:], activated], axis=1),
        jnp.concatenate(
            [late[:, :features], jnp.zeros((count, 2 * features), bf16), late[:, features:]], axis=1
        ),
    )
    spread = columns.reshape(count, n, own_rows).transpose(1, 0, 2)
    own_columns = lax.all_to_all(spread, "dp", 0, 0, tiled=True).reshape(n * count, own_rows)
    others = jnp.stack(
        [mine(grad_branch, npool_t), mine(grad_branch, attended_x), mine(normed_mid, mid_x)]
    )
    others = lax.all_gather(others, "dp", axis=1, tiled=True)

    row_cap = jnp.asarray(np.arange(total)[:, None] // length, jnp.int32)
    col_cap = jnp.asarray(np.tile(np.arange(count), GROUP)[None], jnp.int32)
    kv_part = call(
        key_grad_kernel,
        sds((features, features), f32),
        mine(compact_prob, raw_x), mine(grad_att, queries_x), normed_t, fold, row_cap, col_cap,
        name="key_grad",
    )
    kv_share = summed_slice(kv_part, "dp")
    share_rows = features // n
    slots = own_rows // share_rows
    holder = {share_of(i, n): i for i in range(n)}
    placed = []
    for s in range(slots):
        route = []
        for owner in range(2 * n):
            row = owner * own_rows + s * share_rows
            if features <= row < 3 * features:
                tower, at = divmod((row - features) // share_rows, n)
                route.append((tower * n + holder[at], owner))
        placed.append(lax.ppermute(kv_share, both, route))
    kv_rows = jnp.concatenate(placed, axis=0)

    first_row = (lax.axis_index("tower") * n + index) * own_rows
    last_row = first_row + own_rows - 1
    up_row, down_row = 4 * features, 4 * features + hidden_units

    def other_of(row):
        in_low = jnp.where(row < 3 * features, 0, jnp.where(row < up_row, 1, 2))
        return jnp.where(row >= down_row, 0, in_low)

    edges = jnp.array([features, 3 * features, up_row, down_row], jnp.int32)
    inside = (edges > first_row) & (edges <= last_row)
    edge = jnp.min(jnp.where(inside, edges - first_row, own_rows))
    info = jnp.stack(
        [
            other_of(first_row), other_of(last_row), edge, first_row,
            jnp.int32(features), jnp.int32(3 * features),
        ]
    ).astype(jnp.int32)
    own_grads, squares = pl.pallas_call(
        owner_kernel,
        grid_spec=pltpu.PrefetchScalarGridSpec(
            num_scalar_prefetch=1,
            grid=(1,),
            in_specs=[
                pl.BlockSpec((n * count, own_rows), lambda i, s: (0, 0)),
                pl.BlockSpec((1, n * count, features), lambda i, s: (s[0], 0, 0)),
                pl.BlockSpec((1, n * count, features), lambda i, s: (s[1], 0, 0)),
            ],
            out_specs=(
                pl.BlockSpec((own_rows, features), lambda i, s: (0, 0)),
                pl.BlockSpec((1, features), lambda i, s: (0, 0)),
            ),
        ),
        out_shape=(sds((own_rows, features), f32), sds((1, features), f32)),
        name="owner",
    )(info, own_columns, others, others)

    squares = squares + jnp.sum(kv_share * kv_share, axis=0, keepdims=True)
    sums = jnp.where(text, sums, 0.0)
    sums = summed(jnp.concatenate([sums[:4], squares, sums[5:]], axis=0))
    total_norm_grads = sums[:4]
    grad_norm = jnp.sqrt(jnp.sum(sums[4]) + jnp.sum(total_norm_grads * total_norm_grads))
    factor = jnp.minimum(1.0, CLIP_NORM / (grad_norm + 1e-06))
    grads = (own_grads + kv_rows) * factor
    norm_grads = total_norm_grads * factor
    step_rate = 0.4 * math.sqrt(all_rows)
    decayed = grads + DECAY_RATE * weights
    new_momentum = MOMENTUM_RATE * momentum + decayed
    new_weights = weights - step_rate * (decayed + MOMENTUM_RATE * new_momentum)
    new_averages = AVERAGE_RATE * averages + (1.0 - AVERAGE_RATE) * new_weights
    new_norm_momentum = MOMENTUM_RATE * norm_momentum + norm_grads
    new_norm_params = norm_params - step_rate * (norm_grads + MOMENTUM_RATE * new_norm_momentum)
    new_norm_averages = AVERAGE_RATE * norm_averages + (1.0 - AVERAGE_RATE) * new_norm_params
    input_grad = jnp.where(text, right, left_x.astype(f32)).reshape(caps, length, half)
    return (
        grads,
        norm_grads,
        input_grad,
        new_weights,
        new_momentum,
        new_averages,
        new_norm_params,
        new_norm_momentum,
        new_norm_averages,
        grad_norm,
    )


def solution(mesh):
    return jax.shard_map(
        local,
        mesh=mesh,
        in_specs=(
            P("dp", None, None),
            P("dp", None, None),
            P("dp", None),
            P("dp"),
            P("dp"),
            P("dp", None),
            P(),
            P(("tower", "dp"), None),
            P(),
            P(("tower", "dp"), None),
            P(),
            P(("tower", "dp"), None),
            P(),
        ),
        out_specs=(
            P(("tower", "dp"), None),
            P(),
            P("dp", None, "tower"),
            P(("tower", "dp"), None),
            P(("tower", "dp"), None),
            P(("tower", "dp"), None),
            P(),
            P(),
            P(),
            P(),
        ),
        check_vma=False,
    )
```

```python
from functools import partial
import math

import jax
import jax.numpy as jnp
import numpy as np
from jax import lax
from jax.experimental import pallas as pl
from jax.experimental.pallas import tpu as pltpu
from jax.sharding import PartitionSpec as P

HEAD_DIM = 64
GROUP = 4

EPSILON = 1e-06
LOGIT_SCALE = 50.0
CLIP_NORM = 1.0
MOMENTUM_RATE = 0.9
DECAY_RATE = 0.0001
AVERAGE_RATE = 0.7
MASKED = -1e30
GELU_A = 0.044715
GELU_C = math.sqrt(2.0 / math.pi)

POS_TEXT, POS_IMAGE, LOW, HIGH, PLACE, COUNT_PLACE, SLOT, REAL = range(8)

f32 = jnp.float32
bf16 = jnp.bfloat16


def round_up(value, step):
    return (value + step - 1) // step * step


def dot_nn(left, right, **kw):
    return lax.dot_general(
        left, right, (((1,), (0,)), ((), ())), preferred_element_type=f32, **kw
    )


def dot_nt(left, right):
    return lax.dot_general(left, right, (((1,), (1,)), ((), ())), preferred_element_type=f32)


def dot_tn(left, right):
    return lax.dot_general(left, right, (((0,), (0,)), ((), ())), preferred_element_type=f32)


def call(
    kernel, outs, *args, scratch=(), name=None, weights=None, smem=None, micros=5, in_hbm=False,
    aliases=None,
):
    space = pl.BlockSpec(memory_space=pltpu.HBM if in_hbm else pltpu.VMEM)
    specs = [space] * len(args)
    if smem is not None:
        specs = [pl.BlockSpec(memory_space=pltpu.SMEM)] + specs
        args = (smem, *args)
    if weights is not None:
        parts, table = weights
        specs = (
            [pl.BlockSpec(memory_space=pltpu.SMEM)]
            + [pl.BlockSpec(memory_space=pltpu.HBM)] * len(parts)
            + specs
        )
        args = (table, *parts, *args)
    return pl.pallas_call(
        kernel,
        out_shape=outs,
        in_specs=specs,
        out_specs=jax.tree.map(lambda _: space, outs),
        scratch_shapes=list(scratch),
        input_output_aliases=aliases or {},
        cost_estimate=pl.CostEstimate(
            flops=micros * 1_000_000_000, bytes_accessed=micros * 2_000_000, transcendentals=0
        ),
        name=name,
    )(*args)


def sds(shape, dtype):
    return jax.ShapeDtypeStruct(shape, dtype)


def normalize(rows):
    middle = jnp.mean(rows, axis=-1, keepdims=True)
    centred = rows - middle
    spread = jnp.mean(centred * centred, axis=-1, keepdims=True)
    scale = lax.rsqrt(spread + EPSILON)
    return centred * scale, scale


def norm_pull(grad, rows, gain):
    unit, scale = normalize(rows)
    scaled = grad * gain
    pulled = scale * (
        scaled
        - jnp.mean(scaled, axis=-1, keepdims=True)
        - unit * jnp.mean(scaled * unit, axis=-1, keepdims=True)
    )
    return pulled, grad * unit


def lanes_of_heads(count):
    return lax.broadcasted_iota(jnp.int32, (count, GROUP * HEAD_DIM), 1) // HEAD_DIM


def stack_heads(block):
    lanes = lanes_of_heads(block.shape[0])
    zero = jnp.zeros_like(block)
    return jnp.concatenate([jnp.where(lanes == h, block, zero) for h in range(GROUP)], axis=0)


def unstack_heads(block):
    count = block.shape[0] // GROUP
    lanes = lanes_of_heads(count)
    total = jnp.where(lanes == 0, block[:count], 0.0)
    for h in range(1, GROUP):
        total = jnp.where(lanes == h, block[h * count : (h + 1) * count], total)
    return total


def group_slice(index, base=0):
    return pl.ds(pl.multiple_of(base + index * 256, 256), 256)


def rows_kernel(
    step, text_ref, captions_ref, images_ref, facts_ref, norms_t_ref, norms_i_ref,
    normed_t_ref, normed_ref, npool_t_ref, npool_ref, xpool_ref, facts_out_ref, norms_ref,
):
    facts_out_ref[...] = facts_ref[...]
    norms_ref[...] = jnp.where(text_ref[0] == 1, norms_t_ref[...], norms_i_ref[...])

    def pooled(x_ref, fact, from_ref, to_ref):
        count = to_ref.shape[0]
        pick = (
            lax.broadcasted_iota(jnp.int32, (count, x_ref.shape[0]), 1)
            == facts_ref[:, fact : fact + 1]
        ).astype(bf16)
        to_ref[...] = dot_nn(pick, from_ref[...]).astype(bf16)
        xpool_ref[...] = dot_nn(pick, x_ref[...])

    @pl.loop(0, captions_ref.shape[0] // step)
    def _(i):
        here = pl.ds(pl.multiple_of(i * step, step), step)
        unit, _ = normalize(captions_ref[here, :].astype(f32))
        normed_t_ref[here, :] = (unit * norms_t_ref[0:1, :] + norms_t_ref[1:2, :]).astype(bf16)

    pooled(captions_ref, POS_TEXT, normed_t_ref, npool_t_ref)

    @pl.when(text_ref[0] == 1)
    def _():
        normed_ref[...] = normed_t_ref[...]
        npool_ref[...] = npool_t_ref[...]

    @pl.when(text_ref[0] == 0)
    def _():
        @pl.loop(0, images_ref.shape[0] // step)
        def _(i):
            here = pl.ds(pl.multiple_of(i * step, step), step)
            unit, _ = normalize(images_ref[here, :].astype(f32))
            normed_ref[here, :] = (unit * norms_i_ref[0:1, :] + norms_i_ref[1:2, :]).astype(bf16)

        pooled(images_ref, POS_IMAGE, normed_ref, npool_ref)


class Waits:
    def __init__(self, waits, size):
        self.waits, self.size, self.done = waits, size, set()

    def __call__(self, low, high):
        for u in range(low // self.size, -(-high // self.size)):
            if u not in self.done:
                self.done.add(u)
                self.waits[u]()


def attend_kernel(parts, table_ref, *refs):
    part_refs = refs[:parts]
    (
        normed_ref, npool_ref, xpool_ref, norms_ref, facts_ref, fold_ref,
        q_ref, k_ref, v_ref, probs_ref, folded_ref, att_ref, hidden_ref, nm_ref, w_ref, sems,
    ) = refs[parts:]
    count, features = npool_ref.shape
    total = normed_ref.shape[0]
    need = Waits(
        fetch(table_ref, part_refs, 0, 4 * features, w_ref, sems), part_refs[0].shape[0]
    )
    keys = lax.broadcasted_iota(jnp.int32, (count, total), 1)
    allowed = ((keys >= facts_ref[:, LOW : LOW + 1]) & (keys < facts_ref[:, HIGH : HIGH + 1]))[None]
    need(0, features)
    q_ref[...] = dot_nt(npool_ref[...], w_ref[pl.ds(0, features), :]).astype(bf16)
    for to_ref, base in ((k_ref, features), (v_ref, 2 * features)):
        need(base, base + features)
        wide = features // 2

        @pl.loop(0, 2)
        def _(i, to_ref=to_ref, base=base):
            here = pl.ds(pl.multiple_of(i * wide, 128), wide)
            from_rows = pl.ds(pl.multiple_of(base + i * wide, 128), wide)
            to_ref[:, here] = dot_nt(normed_ref[...], w_ref[from_rows, :]).astype(bf16)

    @pl.loop(0, features // 256)
    def _(i):
        cols = group_slice(i)
        scores = dot_nt(stack_heads(q_ref[:, cols]), k_ref[:, cols]) * HEAD_DIM**-0.5
        scores = jnp.where(allowed, scores.reshape(GROUP, count, total), MASKED)
        exponent = jnp.exp(scores - jnp.max(scores, axis=-1, keepdims=True))
        probs = exponent / jnp.sum(exponent, axis=-1, keepdims=True)
        probs = probs.reshape(GROUP * count, total)
        probs_ref[i] = probs
        low = probs.astype(bf16)
        att_ref[:, cols] = unstack_heads(dot_nn(low, v_ref[:, cols])).astype(bf16)
        folded_ref[i] = dot_nt(fold_ref[...], low).astype(bf16)

    need(3 * features, 4 * features)
    hidden = xpool_ref[...] + dot_nt(
        att_ref[...], w_ref[pl.ds(3 * features, features), :]
    )
    hidden_ref[...] = hidden
    unit, _ = normalize(hidden)
    nm_ref[...] = (unit * norms_ref[2:3, :] + norms_ref[3:4, :]).astype(bf16)


def gelu_parts(pre):
    tanh = jnp.tanh(GELU_C * (pre + GELU_A * pre * pre * pre))
    return 0.5 * (1.0 + tanh), tanh


def feed_kernel(parts, first, skip, blocks, images, table_ref, *refs):
    part_refs = refs[:parts]
    (
        text_ref, nm_ref, hidden_ref, count_ref,
        pre_ref, act_ref, pooled_ref, inverse_ref, emb_ref, w_ref, total_ref, sems,
    ) = refs[parts:]
    units = pre_ref.shape[1]
    block = units // blocks
    need = Waits(
        fetch(table_ref, part_refs, first, w_ref.shape[0], w_ref, sems), part_refs[0].shape[0]
    )
    for i in range(blocks):
        here = pl.ds(i * block, block)
        up, down = skip + i * block, skip + units + i * block
        need(up, up + block)
        pre = dot_nt(nm_ref[...], w_ref[pl.ds(up, block), :])
        pre_ref[:, here] = pre
        act = (pre * gelu_parts(pre)[0]).astype(bf16)
        act_ref[:, here] = act
        need(down, down + block)
        part = dot_nn(act, w_ref[pl.ds(down, block), :])
        total_ref[...] = part + (hidden_ref[...] if i == 0 else total_ref[...])

    need(0, w_ref.shape[0])
    pooled = total_ref[...]
    inverse = lax.rsqrt(jnp.sum(pooled * pooled, axis=-1, keepdims=True) + EPSILON)
    pooled_ref[...] = pooled
    inverse_ref[...] = jnp.broadcast_to(inverse, inverse_ref.shape)
    emb = pooled * inverse
    counted = (lax.broadcasted_iota(jnp.int32, emb.shape, 0) == images) & (text_ref[0] == 0)
    emb_ref[...] = jnp.where(counted, count_ref[...], emb).astype(bf16)


def loss_kernel(
    chunk, text_a_ref, text_b_ref, img_a_ref, img_b_ref, row_bias_ref, col_bias_ref,
    emb_ref, pooled_ref, inverse_ref, facts_ref, grad_ref, branch_ref, img_ref,
):
    images = img_ref.shape[0]
    count = emb_ref.shape[0]
    img_ref[pl.ds(0, images // 2), :] = img_a_ref[...]
    img_ref[pl.ds(images // 2, images // 2), :] = img_b_ref[...]
    top, acc = jnp.full((1, images), MASKED, f32), jnp.zeros((1, images), f32)
    for text_ref in (text_a_ref, text_b_ref):

        def body(j, carry, text_ref=text_ref):
            top, acc = carry
            here = pl.ds(pl.multiple_of(j * chunk, 8), chunk)
            logits = LOGIT_SCALE * dot_nt(text_ref[here, :], img_ref[...]) + row_bias_ref[...]
            higher = jnp.maximum(top, jnp.max(logits, axis=0, keepdims=True))
            acc = acc * jnp.exp(top - higher) + jnp.sum(
                jnp.exp(logits - higher), axis=0, keepdims=True
            )
            return higher, acc

        top, acc = lax.fori_loop(0, text_ref.shape[0] // chunk, body, (top, acc))

    column_lse = top + jnp.log(acc)
    logits = LOGIT_SCALE * dot_nt(emb_ref[...], img_ref[...])
    masked = logits + col_bias_ref[...]
    row_top = jnp.max(masked, axis=1, keepdims=True)
    row_exp = jnp.exp(masked - row_top)
    by_row = row_exp / jnp.sum(row_exp, axis=1, keepdims=True)
    by_column = jnp.exp(masked - column_lse)
    columns = lax.broadcasted_iota(jnp.int32, (count, images), 1)
    target = (columns == facts_ref[:, PLACE : PLACE + 1]).astype(f32)
    listed = dot_nn((columns == facts_ref[:, COUNT_PLACE : COUNT_PLACE + 1]).astype(bf16), img_ref[...])
    at = lax.broadcasted_iota(jnp.int32, listed.shape, 1) == facts_ref[:, SLOT : SLOT + 1]
    named = jnp.maximum(jnp.sum(jnp.where(at, listed, 0.0), axis=1, keepdims=True), 1.0)
    grad_logits = 0.5 * (by_row - target) + 0.5 * (by_column - target / named)
    scaled = jnp.where(
        (col_bias_ref[...] == 0.0) & (facts_ref[:, REAL : REAL + 1] > 0), LOGIT_SCALE * grad_logits, 0.0
    ).astype(bf16)
    grad_embed = dot_nn(scaled, img_ref[...])
    pooled = pooled_ref[...]
    inverse = inverse_ref[:, 0:1]
    projection = jnp.sum(pooled * grad_embed, axis=-1, keepdims=True)
    grad_pooled = inverse * grad_embed - inverse * inverse * inverse * projection * pooled
    grad_ref[...] = grad_pooled
    branch_ref[...] = grad_pooled.astype(bf16)


def feed_back_kernel(parts, first, skip, blocks, table_ref, *refs):
    part_refs = refs[:parts]
    (
        branch_ref, grad_ref, hidden_ref, norms_ref, pre_ref,
        gpre_ref, ghidden_ref, mixed_ref, sums_ref, gatt_ref, w_ref, total_ref, sems,
    ) = refs[parts:]
    units = pre_ref.shape[1]
    features = branch_ref.shape[1]
    block = units // blocks
    need = Waits(
        fetch(table_ref, part_refs, first, w_ref.shape[0], w_ref, sems), part_refs[0].shape[0]
    )
    for i in range(blocks):
        here = pl.ds(i * block, block)
        up, down = skip + i * block, skip + units + i * block
        pre = pre_ref[:, here]
        cdf, tanh = gelu_parts(pre)
        slope = cdf + pre * 0.5 * (1.0 - tanh * tanh) * GELU_C * (1.0 + 3.0 * GELU_A * pre * pre)
        need(down, down + block)
        grad_act = dot_nt(branch_ref[...], w_ref[pl.ds(down, block), :]).astype(bf16)
        gpre = (grad_act.astype(f32) * slope).astype(bf16)
        gpre_ref[:, here] = gpre
        need(up, up + block)
        part = dot_nn(gpre, w_ref[pl.ds(up, block), :])
        total_ref[...] = part if i == 0 else part + total_ref[...]

    need(0, w_ref.shape[0])
    grad = total_ref[...]
    pulled, by_gain = norm_pull(grad, hidden_ref[...], norms_ref[2:3, :])
    ghidden = grad_ref[...] + pulled
    mixed = ghidden.astype(bf16)
    ghidden_ref[...] = ghidden
    mixed_ref[...] = mixed
    gatt_ref[...] = dot_nn(mixed, w_ref[pl.ds(skip - features, features), :]).astype(bf16)
    sums_ref[...] = jnp.zeros_like(sums_ref)
    sums_ref[2:3, :] = jnp.sum(by_gain, axis=0, keepdims=True)
    sums_ref[3:4, :] = jnp.sum(grad, axis=0, keepdims=True)


def three_parts(value):
    high = value.astype(bf16)
    rest = value - high.astype(f32)
    middle = rest.astype(bf16)
    low = (rest - middle.astype(f32)).astype(bf16)
    return jnp.concatenate([high, middle, low], axis=0)


def attend_back_kernel(parts, step, half, table_ref, *refs):
    part_refs = refs[:parts]
    (
        text_ref, gatt_ref, ghidden_ref, probs_ref, q_ref, k_ref, v_ref, x_ref, normed_ref, facts_ref,
        norms_ref, sums_in_ref,
        gq_ref, left_ref, right_ref, sums_ref, key_ref, joined_ref, grad_ref, w_ref, sems,
    ) = refs[parts:]
    count, features = gatt_ref.shape

    @pl.when(text_ref[0] == 1)
    def _():
        need = Waits(
            fetch(table_ref, part_refs, 0, 3 * features, w_ref, sems), part_refs[0].shape[0]
        )

        @pl.loop(0, features // 256)
        def _(i):
            cols = group_slice(i)
            gatt = stack_heads(gatt_ref[:, cols])
            queries = stack_heads(q_ref[:, cols])
            key_rows, values = k_ref[:, cols], v_ref[:, cols]
            probs = probs_ref[i]
            grad_probs = dot_nt(gatt, values)
            mean = jnp.sum(probs * grad_probs, axis=-1, keepdims=True)
            raw = (probs * (grad_probs - mean) * HEAD_DIM**-0.5).astype(bf16)
            gq_ref[:, cols] = unstack_heads(dot_nn(raw, key_rows)).astype(bf16)
            joined_ref[:, cols] = dot_tn(raw, queries).astype(bf16)
            joined_ref[:, group_slice(i, features)] = dot_tn(probs.astype(bf16), gatt).astype(bf16)

        need(0, 3 * features)
        gpool = dot_nn(gq_ref[...], w_ref[pl.ds(0, features), :])
        extra = jnp.concatenate([three_parts(gpool), three_parts(ghidden_ref[...])], axis=1)
        gain = norms_ref[0:1, :]
        places = facts_ref[POS_TEXT : POS_TEXT + 1, :]
        places = jnp.concatenate([places, places, places], axis=1)

        def body(j, carry):
            dgain, doffset = carry
            here = pl.ds(pl.multiple_of(j * step, 16), step)
            pick = (
                lax.broadcasted_iota(jnp.int32, (step, 3 * count), 0) + j * step == places
            ).astype(bf16)
            added = dot_nn(pick, extra)
            grad = (
                dot_nn(joined_ref[here, :], w_ref[pl.ds(features, 2 * features), :])
                + added[:, :features]
            )
            pulled, by_gain = norm_pull(grad, x_ref[here, :].astype(f32), gain)
            pulled = pulled + added[:, features:]
            left_ref[here, :] = pulled[:, :half].astype(bf16)
            right_ref[here, :] = pulled[:, half:]
            return (
                dgain + jnp.sum(by_gain, axis=0, keepdims=True),
                doffset + jnp.sum(grad, axis=0, keepdims=True),
            )

        none = jnp.zeros((1, features), f32)
        dgain, doffset = lax.fori_loop(0, left_ref.shape[0] // step, body, (none, none))
        sums_ref[...] = sums_in_ref[...]
        sums_ref[0:1, :] = dgain
        sums_ref[1:2, :] = doffset

        @pl.loop(0, features // 256)
        def _(i):
            key_ref[group_slice(i), :] = dot_tn(joined_ref[:, group_slice(i)], normed_ref[...])


def value_grad_kernel(
    text_ref, folded_hbm, factor_hbm, normed_hbm, spread_hbm, row_hbm, col_hbm, _, out_hbm,
    folded_ref, factor_ref, normed_ref, spread_ref, row_ref, col_ref, out_ref, sems,
):
    features = factor_ref.shape[1]

    @pl.when(text_ref[0] == 0)
    def _():
        moves = [
            pltpu.make_async_copy(from_hbm, to_ref, sems.at[i])
            for i, (from_hbm, to_ref) in enumerate(
                (
                    (folded_hbm, folded_ref), (factor_hbm, factor_ref), (normed_hbm, normed_ref),
                    (spread_hbm, spread_ref), (row_hbm, row_ref), (col_hbm, col_ref),
                )
            )
        ]
        for move in moves:
            move.start()
        for move in moves:
            move.wait()

        @pl.loop(0, features // 256)
        def _(i):
            factor = stack_heads(factor_ref[:, group_slice(i)])
            wide = dot_nn(spread_ref[...], folded_ref[i])
            wide = jnp.where(row_ref[...] == col_ref[...], wide, 0.0).astype(bf16)
            joined = dot_nn(wide, factor).astype(bf16)
            out_ref[group_slice(i), :] = dot_tn(joined, normed_ref[...])

        pltpu.sync_copy(out_ref, out_hbm)


def pack_kernel(lower, text_ref, pre_ref, act_ref, query_ref, late_ref, out_ref):
    features = query_ref.shape[1]
    own = out_ref.shape[2]

    def fill(pieces):
        start = 0
        for ref, first, size in pieces:
            at = start
            while at < start + size:
                to = at % own
                taken = min(own - to, start + size - at)
                from_lane = first + at - start
                out_ref[at // own, :, to : to + taken] = ref[:, from_lane : from_lane + taken]
                at += taken
            start += size

    @pl.when(text_ref[0] == 1)
    def _():
        fill([(pre_ref, lower, pre_ref.shape[1] - lower), (act_ref, 0, act_ref.shape[1])])

    @pl.when(text_ref[0] == 0)
    def _():
        first, last = features // own, 3 * features // own
        out_ref[first : last + 1] = jnp.zeros((last + 1 - first,) + out_ref.shape[1:], bf16)
        fill([(query_ref, 0, features)])
        start = 3 * features
        at = 0
        while at < features + lower:
            to = (start + at) % own
            taken = min(own - to, features + lower - at)
            out_ref[(start + at) // own, :, to : to + taken] = late_ref[:, at : at + taken]
            at += taken


def owner_kernel(info_ref, a_ref, b0_ref, b1_ref, sums_ref, out_ref, stats_ref):
    rows = lax.broadcasted_iota(jnp.int32, out_ref.shape, 0)
    edge = info_ref[2]
    out_ref[...] = dot_tn(a_ref[...], b0_ref[0])

    @pl.when(edge < out_ref.shape[0])
    def _():
        out_ref[...] = jnp.where(rows < edge, out_ref[...], dot_tn(a_ref[...], b1_ref[0]))

    place = rows + info_ref[3]
    grad = jnp.where((place < info_ref[4]) | (place >= info_ref[5]), out_ref[...], 0.0)
    out_ref[...] = grad
    at = lax.broadcasted_iota(jnp.int32, stats_ref.shape, 0)
    known = jnp.where((at < 4) & (info_ref[6] == 1), sums_ref[...], 0.0)
    stats_ref[...] = jnp.where(at == 4, jnp.sum(grad * grad, axis=0, keepdims=True), known)


def update_kernel(
    step_rate, slots, stats_ref, own_ref, *refs,
):
    placed_refs = refs[:slots]
    (
        weights_ref, momentum_ref, averages_ref, norms_ref, norm_momentum_ref, norm_averages_ref,
        grads_ref, new_weights_ref, new_momentum_ref, new_averages_ref,
        norm_grads_ref, new_norms_ref, new_norm_momentum_ref, new_norm_averages_ref, norm_ref,
    ) = refs[slots:]
    sums = stats_ref[0:4, :]
    total = jnp.sum(stats_ref[4:5, :], axis=1, keepdims=True) + jnp.sum(
        jnp.sum(sums * sums, axis=1, keepdims=True), axis=0, keepdims=True
    )
    grad_norm = jnp.sqrt(total)
    factor = jnp.minimum(1.0, CLIP_NORM / (grad_norm + 1e-06))
    norm_ref[...] = grad_norm

    def moved(grad, decayed, old, old_momentum, old_average):
        new_momentum = MOMENTUM_RATE * old_momentum + decayed
        new = old - step_rate * (decayed + MOMENTUM_RATE * new_momentum)
        return new, new_momentum, AVERAGE_RATE * old_average + (1.0 - AVERAGE_RATE) * new

    grad = sums * factor
    norm_grads_ref[...] = grad
    new_norms_ref[...], new_norm_momentum_ref[...], new_norm_averages_ref[...] = moved(
        grad, grad, norms_ref[...], norm_momentum_ref[...], norm_averages_ref[...]
    )
    size = own_ref.shape[0] // slots
    for s, placed_ref in enumerate(placed_refs):
        here = slice(s * size, (s + 1) * size)
        grad = (own_ref[here, :] + placed_ref[...]) * factor
        grads_ref[here, :] = grad
        old = weights_ref[here, :]
        new_weights_ref[here, :], new_momentum_ref[here, :], new_averages_ref[here, :] = moved(
            grad, grad + DECAY_RATE * old, old, momentum_ref[here, :], averages_ref[here, :]
        )


def bits_of(axis):
    size = lax.axis_size(axis)
    return [1 << b for b in range(size.bit_length() - 1)]


def swapped(block, axis, bit):
    return lax.ppermute(block, axis, [(i, i ^ bit) for i in range(lax.axis_size(axis))])


UNITS = 16


def units_gathered(low_shard, image_weights, text, prepare):
    n = lax.axis_size("dp")
    chips = n // 2
    steps = chips // 2
    index = lax.axis_index("dp")
    core = index % 2
    other_core = [(i, i ^ 1) for i in range(n)]
    order = list(range(0, chips, 2)) + list(range(1, chips, 2))[::-1]
    seat_of = np.zeros(chips, np.int32)
    seat_of[order] = np.arange(chips)
    route = []
    for s in range(chips):
        route.append((2 * order[s], 2 * order[(s + 1) % chips]))
        route.append((2 * order[s] + 1, 2 * order[s - 1] + 1))

    def pair(own, other):
        return jnp.where(
            core == 0,
            jnp.concatenate([own, other], axis=0),
            jnp.concatenate([other, own], axis=0),
        )

    def swap(block):
        return lax.ppermute(block, "dp", other_core)

    def onward(block):
        return lax.ppermute(block, "dp", route)

    def half_of(block):
        size = block.shape[0] // 2
        return lax.dynamic_slice_in_dim(block, core * size, size, axis=0)

    high = swap(low_shard)
    image = swap(image_weights)
    b_part = jnp.where(text, pair(low_shard, high), jnp.where(core == 0, image, image_weights))
    low_shard, image, image_weights, b_part = lax.optimization_barrier(
        (low_shard, image, image_weights, b_part)
    )
    over = lax.ppermute(low_shard, "tower", [(0, 1)])
    low = swap(over)
    a_part = jnp.where(text, pair(over, low), jnp.where(core == 0, image_weights, image))

    unit = np.arange(UNITS)
    part = jnp.where(text, unit // chips, unit % 2)
    far = (seat_of[None] - seat_of[:, None]) % chips
    own_far = jnp.sum(
        jnp.where(jnp.arange(chips)[None] == index // 2, jnp.asarray(far), 0), axis=1
    )
    far = jnp.where(text, jnp.tile(own_far, 2), jnp.repeat(own_far, 2))
    step = jnp.minimum(far, chips - far)
    from_other = (far < steps) == (core == 1)
    table = jnp.where(
        far == 0,
        part,
        jnp.where(
            far == steps,
            4 * steps - 2 + 2 * part + core,
            4 * step - 2 + part + 2 * from_other,
        ),
    ).astype(jnp.int32)

    parts = [a_part, b_part]
    sent_a, sent_b = a_part, b_part
    prepared = prepare(b_part)
    for step in range(1, steps):
        sent_b = onward(sent_b)
        if step == 1:
            sent_a, sent_b = lax.optimization_barrier((sent_a, sent_b))
        elif step == 2:
            sent_a, prepared, table = lax.optimization_barrier((sent_a, prepared, table))
        sent_a = onward(sent_a)
        parts += [sent_a, sent_b, swap(sent_a), swap(sent_b)]
    last_b = onward(half_of(sent_b))
    last_a = onward(half_of(sent_a))
    parts += [last_a, swap(last_a), last_b, swap(last_b)]
    return parts, table, prepared


def fetch(table_ref, part_refs, first, rows, to_ref, sems):
    size = part_refs[0].shape[0]
    half = size // 2
    whole = [p for p in part_refs if p.shape[0] == size]
    halves = part_refs[len(whole) :]
    waits = []
    for u in range(-(-rows // size)):
        taken = min(size, rows - u * size)

        def copy(from_ref, at, count, u=u):
            return pltpu.make_async_copy(
                from_ref.at[pl.ds(0, count), :], to_ref.at[pl.ds(u * size + at, count), :], sems.at[u]
            )

        for j, part_ref in enumerate(whole):

            @pl.when(table_ref[first + u] == j)
            def _(part_ref=part_ref):
                copy(part_ref, 0, taken).start()

        for j in range(len(halves)):

            @pl.when(table_ref[first + u] == len(whole) + j)
            def _(j=j):
                mine, other = halves[j // 2 * 2], halves[j // 2 * 2 + 1]
                upper, lower = (mine, other) if j % 2 == 0 else (other, mine)
                copy(upper, 0, min(half, taken)).start()
                if taken > half:
                    copy(lower, half, taken - half).start()

        waits.append(copy(whole[0], 0, taken).wait)
    return waits


def stages_of(axis):
    size = lax.axis_size(axis)
    if size == 16:
        return [(4, 8), (2,), (1,)]
    return [(bit,) for bit in reversed(bits_of(axis))]


def gather_stage(block, axis, stage):
    blocks = [block]
    for bit in range(1, 1 << len(stage)):
        other = sum(b for s, b in enumerate(stage) if bit >> s & 1)
        blocks.append(swapped(block, axis, other))
    return blocks


def place_in_gathered(device, axis):
    other = lax.axis_index(axis) ^ device
    order = [bit for stage in stages_of(axis) for bit in stage]
    return sum(((other & bit) // bit) << s for s, bit in enumerate(order))


def share_step(block, axis, bit, others=()):
    levels = lax.axis_size(axis).bit_length() - 1
    dim = levels - bit.bit_length()
    mine = ((lax.axis_index(axis) & bit) != 0).astype(jnp.int32)
    kept = lax.dynamic_slice_in_dim(block, mine, 1, axis=dim)
    sent = lax.dynamic_slice_in_dim(block, 1 - mine, 1, axis=dim)
    received, others = lax.optimization_barrier((swapped(sent, axis, bit), others))
    return kept + received, others


def summed(block, others):
    size = lax.axis_size("dp")
    if size != 16:
        for axis in ("dp", "tower"):
            for bit in bits_of(axis):
                block = block + swapped(block, axis, bit)
        return block, others
    across = [(t * size + i, (1 - t) * size + (i ^ 2)) for t in range(2) for i in range(size)]
    block = (block + lax.ppermute(block, "tower", [(0, 1), (1, 0)])) + (
        swapped(block, "dp", 2) + lax.ppermute(block, ("tower", "dp"), across)
    )
    block = (block + swapped(block, "dp", 4)) + (
        swapped(block, "dp", 8) + swapped(block, "dp", 12)
    )
    other, others = lax.optimization_barrier((swapped(block, "dp", 1), others))
    return block + other, others


def local(
    images,
    captions,
    token_ids,
    counts,
    matches,
    image_weights,
    image_norms,
    weights,
    norm_params,
    momentum,
    norm_momentum,
    averages,
    norm_averages,
):
    text = lax.axis_index("tower") == 1
    index = lax.axis_index("dp")
    n = lax.axis_size("dp")
    both = ("tower", "dp")
    caps, length, features = captions.shape
    imgs, img_rows = images.shape[:2]
    text_rows = caps * length
    own_rows = weights.shape[0]
    all_rows = 2 * n * own_rows
    hidden_units = (all_rows - 4 * features) // 2
    count = round_up(max(caps, imgs), 8)
    total = round_up(max(text_rows, imgs * img_rows), 48)
    wide = GROUP * count

    def mine(of_text, of_image):
        return jnp.where(text, of_text, of_image)

    def padded_to(values, fill):
        return jnp.pad(values, (0, count - values.shape[0]), constant_values=fill)

    def padded(rows):
        return jnp.pad(rows.reshape(-1, features), ((0, total - rows.shape[0] * rows.shape[1]), (0, 0)))

    img_slots = round_up(imgs + 1, 8)

    def prepare(ready):
        caption_in, image_in, ids, named, tallies, _ = lax.optimization_barrier(
            (captions, images, token_ids, matches, counts, ready)
        )
        caption_x = padded(caption_in)
        lengths = jnp.sum((ids != 0).astype(jnp.int32), axis=1)
        start_t = jnp.arange(caps, dtype=jnp.int32) * length
        start_i = jnp.arange(imgs, dtype=jnp.int32) * img_rows
        pos_t = start_t + lengths - 1
        owner_place = place_in_gathered(named // imgs, "dp")
        columns = [
            padded_to(pos_t, 0),
            padded_to(start_i, 0),
            mine(padded_to(start_t, 0), padded_to(start_i, 0)),
            mine(padded_to(start_t + lengths, 1), padded_to(start_i + img_rows, 1)),
            padded_to(owner_place * img_slots + named % imgs, 0),
            padded_to(owner_place * img_slots + imgs, 0),
            padded_to(named % imgs, 0),
            jnp.asarray(np.arange(count) < caps, jnp.int32),
        ]
        facts = jnp.stack(columns, axis=0)
        table = jnp.pad(facts.T, ((0, 0), (0, 128 - len(columns))))
        rows = call(
            partial(rows_kernel, 48),
            (
                sds((total, features), bf16),
                sds((total, features), bf16),
                sds((count, features), bf16),
                sds((count, features), bf16),
                sds((count, features), f32),
                sds((count, 128), jnp.int32),
                sds((4, features), f32),
            ),
            caption_x, padded(image_in), table, norm_params, image_norms,
            smem=text.astype(jnp.int32)[None],
            name="rows",
        )
        first_row = (lax.axis_index("tower") * n + index) * own_rows
        last_row = first_row + own_rows - 1
        up_row, down_row = 4 * features, 4 * features + hidden_units

        def other_of(row):
            in_low = jnp.where(row < 3 * features, 0, jnp.where(row < up_row, 1, 2))
            return jnp.where(row >= down_row, 0, in_low)

        edge = jnp.int32(own_rows)
        for boundary in (features, 3 * features, up_row, down_row):
            inside = (boundary > first_row) & (boundary <= last_row)
            edge = jnp.where(inside, boundary - first_row, edge)
        info = jnp.stack(
            [
                other_of(first_row), other_of(last_row), edge, first_row,
                jnp.int32(features), jnp.int32(3 * features), text.astype(jnp.int32),
            ]
        ).astype(jnp.int32)
        count_row = jnp.pad(tallies.astype(f32), (0, features - imgs))[None]
        return caption_x, facts, rows, count_row, info

    low_shard = weights.astype(bf16)
    if n == UNITS:
        parts, table, prepared = units_gathered(low_shard, image_weights, text, prepare)
    else:
        even = lax.ppermute(low_shard, both, [(2 * k, n + k) for k in range(n)])
        odd = lax.ppermute(low_shard, both, [(2 * k + 1, n + k) for k in range(n)])
        shard = jnp.where(text, jnp.concatenate([even, odd], axis=0), image_weights)
        packed = lax.all_gather(shard, "dp", axis=0, tiled=True)
        parts = jnp.split(packed, UNITS, axis=0)
        table = jnp.arange(UNITS, dtype=jnp.int32)
        prepared = prepare(shard)
    caption_x, facts, rows, count_row, info = prepared
    normed_t, normed, npool_t, npool, xpool, facts_by_row, norms = rows
    part_rows = all_rows // UNITS
    feed_part = 4 * features // part_rows
    feed_skip = 4 * features - feed_part * part_rows

    flag = text.astype(jnp.int32)[None]
    groups = features // 256
    fold = np.arange(length)[:, None] == np.arange(total)[None] % length
    weights_of = (parts, table)

    def loads(rows):
        return [
            pltpu.VMEM((rows, features), bf16),
            pltpu.SemaphoreType.DMA((-(-rows // part_rows),)),
        ]

    queries, key_rows, values, probs, folded, attended, hidden, normed_mid = call(
        partial(attend_kernel, len(parts)),
        (
            sds((count, features), bf16),
            sds((total, features), bf16),
            sds((total, features), bf16),
            sds((groups, wide, total), f32),
            sds((groups, length, wide), bf16),
            sds((count, features), bf16),
            sds((count, features), f32),
            sds((count, features), bf16),
        ),
        normed, npool, xpool, norms, facts_by_row, jnp.asarray(fold, bf16),
        scratch=loads(4 * features),
        weights=weights_of,
        micros=10,
        name="attend",
    )
    to_image = [(1, 0)]
    early_x = lax.ppermute(jnp.concatenate([attended, normed_mid], axis=1), "tower", to_image)
    folded_x = lax.ppermute(folded, "tower", to_image)
    feed_rows = 2 * hidden_units + feed_skip
    total_scratch = pltpu.VMEM((count, features), f32)

    def feed_scratch(rows):
        weights_at, sems = loads(rows)
        return [weights_at, total_scratch, sems]

    pre_act, activated, pooled, inverse, emb = call(
        partial(feed_kernel, len(parts), feed_part, feed_skip, 2, imgs),
        (
            sds((count, hidden_units), f32),
            sds((count, hidden_units), bf16),
            sds((count, features), f32),
            sds((count, 128), f32),
            sds((count, features), bf16),
        ),
        normed_mid, hidden, count_row,
        smem=flag,
        scratch=feed_scratch(feed_rows),
        weights=weights_of,
        micros=6,
        name="feed",
    )

    emb, early_x, folded_x = lax.optimization_barrier((emb, early_x, folded_x))

    stages = stages_of("dp")
    blocks = gather_stage(emb, "dp", stages[0])
    all_images = lax.ppermute(
        jnp.concatenate([b[:img_slots] for b in blocks], axis=0), "tower", [(0, 1)]
    )
    all_text = jnp.concatenate(blocks, axis=0)
    for stage in stages[1:-1]:
        all_text = jnp.concatenate(gather_stage(all_text, "dp", stage), axis=0)
        all_images = jnp.concatenate(gather_stage(all_images, "dp", stage), axis=0)
    all_text = gather_stage(all_text, "dp", stages[-1])
    all_images = gather_stage(all_images, "dp", stages[-1])
    chunk = count * min(8, n // 2)
    row_bias = np.tile(np.where(np.arange(count) < caps, 0.0, MASKED), chunk // count)[:, None]
    col_bias = np.tile(np.where(np.arange(img_slots) < imgs, 0.0, MASKED), n)[None]
    grad_rows, grad_branch = call(
        partial(loss_kernel, chunk),
        (sds((count, features), f32), sds((count, features), bf16)),
        *all_text, *all_images, jnp.asarray(row_bias, f32), jnp.asarray(col_bias, f32),
        emb, pooled, inverse, facts_by_row,
        scratch=[pltpu.VMEM((n * img_slots, features), bf16)],
        name="loss",
    )
    attended_x, mid_x = early_x[:, :features], early_x[:, features:]
    others = jnp.stack(
        [mine(grad_branch, npool_t), mine(grad_branch, attended_x), mine(normed_mid, mid_x)]
    )
    others, grad_branch = lax.optimization_barrier((others, grad_branch))
    others = lax.all_gather(others, "dp", axis=1, tiled=True)

    back_part = 3 * features // part_rows
    back_skip = 4 * features - back_part * part_rows
    back_rows = 2 * hidden_units + back_skip
    grad_pre, grad_hidden, grad_mixed, sums, grad_att = call(
        partial(feed_back_kernel, len(parts), back_part, back_skip, 2),
        (
            sds((count, hidden_units), bf16),
            sds((count, features), f32),
            sds((count, features), bf16),
            sds((8, features), f32),
            sds((count, features), bf16),
        ),
        grad_branch, grad_rows, hidden, norms, pre_act,
        scratch=feed_scratch(back_rows),
        weights=weights_of,
        micros=7,
        name="feed_back",
    )
    lower = all_rows // 2 - 4 * features
    grad_att_x = lax.ppermute(grad_att, "tower", to_image)
    late_x = lax.ppermute(
        jnp.concatenate([grad_mixed, grad_pre[:, :lower]], axis=1), "tower", to_image
    )

    half = features // 2
    step = max(
        s for s in range(16, 305, 16) if text_rows % s == 0
    )
    grad_q, left, right, sums, key_part = call(
        partial(attend_back_kernel, len(parts), step, half),
        (
            sds((count, features), bf16),
            sds((text_rows, half), bf16),
            sds((text_rows, features - half), f32),
            sds((8, features), f32),
            sds((features, features), f32),
        ),
        grad_att, grad_hidden, probs, queries, key_rows, values, caption_x, normed_t, facts, norms,
        sums,
        smem=flag,
        scratch=[
            pltpu.VMEM((total, 2 * features), bf16),
            pltpu.VMEM((8, 128), f32),
            *loads(3 * features),
        ],
        weights=weights_of,
        micros=16,
        name="attend_back",
    )
    grad_q, key_part, grad_att_x, late_x = lax.optimization_barrier(
        (grad_q, key_part, grad_att_x, late_x)
    )
    grad_q_x = lax.ppermute(grad_q, "tower", to_image)

    spread = jnp.asarray(fold.T, bf16)
    row_cap = jnp.asarray(np.arange(total)[:, None] // length, jnp.int32)
    col_cap = jnp.asarray(np.tile(np.arange(count), GROUP)[None], jnp.int32)
    value_in = (folded_x, grad_att_x, normed_t, spread, row_cap, col_cap)
    kv_part = call(
        value_grad_kernel,
        sds((features, features), f32),
        *value_in, key_part,
        smem=flag,
        in_hbm=True,
        aliases={len(value_in) + 1: 0},
        scratch=[
            *[pltpu.VMEM(v.shape, v.dtype) for v in value_in],
            pltpu.VMEM((features, features), f32),
            pltpu.SemaphoreType.DMA((len(value_in),)),
        ],
        name="value_grad",
    )
    share_rows = features // n
    half_share = share_rows // 2
    bits = bits_of("dp")
    kv_part = kv_part.reshape((2,) * len(bits) + (share_rows, features))
    kv_part, _ = share_step(kv_part, "dp", bits[0])
    grad_q_x, late_x, left, kv_part = lax.optimization_barrier((grad_q_x, late_x, left, kv_part))
    upper, under = kv_part[..., :half_share, :], kv_part[..., half_share:, :]
    upper_order, under_order = bits[1:], bits[2:-1] + bits[1:2] + bits[-1:]
    columns = call(
        partial(pack_kernel, lower),
        sds((n, count, own_rows), bf16),
        grad_pre, activated, grad_q_x, late_x,
        smem=flag,
        micros=2,
        name="pack",
    )
    upper, columns = share_step(upper, "dp", upper_order[0], columns)
    under, _ = share_step(under, "dp", under_order[0])
    left_x = lax.ppermute(left, "tower", to_image)
    input_grad = jnp.where(text, right, left_x.astype(f32)).reshape(caps, length, half)
    for up_bit, under_bit in zip(upper_order[1:-1], under_order[1:-1]):
        upper, input_grad = share_step(upper, "dp", up_bit, input_grad)
        under, _ = share_step(under, "dp", under_bit)

    own_columns = lax.all_to_all(columns, "dp", 0, 0, tiled=True)
    whole = lambda shape: pl.BlockSpec(shape, lambda i, s: (0, 0))
    own_grads, stats = pl.pallas_call(
        owner_kernel,
        grid_spec=pltpu.PrefetchScalarGridSpec(
            num_scalar_prefetch=1,
            grid=(1,),
            in_specs=[
                whole((n * count, own_rows)),
                pl.BlockSpec((1, n * count, features), lambda i, s: (s[0], 0, 0)),
                pl.BlockSpec((1, n * count, features), lambda i, s: (s[1], 0, 0)),
                whole((8, features)),
            ],
            out_specs=(whole((own_rows, features)), whole((8, features))),
        ),
        out_shape=(sds((own_rows, features), f32), sds((8, features), f32)),
        cost_estimate=pl.CostEstimate(
            flops=4_000_000_000, bytes_accessed=8_000_000, transcendentals=0
        ),
        name="owner",
    )(
        info, own_columns.reshape(n * count, own_rows), others, others, sums,
    )
    upper, (own_grads, stats) = share_step(upper, "dp", upper_order[-1], (own_grads, stats))
    under, _ = share_step(under, "dp", under_order[-1])
    kv_share = jnp.concatenate([upper, under], axis=-2).reshape(share_rows, features)

    core = index % 2
    kv_other = swapped(kv_share, "dp", 1)
    kv_pair = jnp.where(
        core == 0,
        jnp.concatenate([kv_share, kv_other], axis=0),
        jnp.concatenate([kv_other, kv_share], axis=0),
    )
    slots = own_rows // (2 * share_rows)
    placed = []
    for s in range(slots):
        route = []
        for owner in range(2 * n):
            row = owner * own_rows + 2 * s * share_rows
            if features <= row < 2 * features:
                route.append((n + (row - features) // share_rows + s % 2, owner))
            elif 2 * features <= row < 3 * features:
                route.append(((row - 2 * features) // share_rows + s % 2, owner))
        placed.append(lax.ppermute(kv_pair, both, route))
    kv_square = jnp.sum(kv_share * kv_share, axis=0)
    stats = stats + jnp.where(jnp.arange(8)[:, None] == 4, kv_square[None], 0.0)
    stats, placed = summed(stats, placed)
    rows_f32, small_f32 = sds((own_rows, features), f32), sds((4, features), f32)
    (
        grads, new_weights, new_momentum, new_averages,
        norm_grads, new_norm_params, new_norm_momentum, new_norm_averages, grad_norm,
    ) = call(
        partial(update_kernel, 0.4 * math.sqrt(all_rows), slots),
        (
            rows_f32, rows_f32, rows_f32, rows_f32,
            small_f32, small_f32, small_f32, small_f32, sds((1, 1), f32),
        ),
        stats, own_grads, *placed, weights, momentum, averages,
        norm_params, norm_momentum, norm_averages,
        name="update",
    )
    grad_norm = grad_norm.reshape(())
    return (
        grads,
        norm_grads,
        input_grad,
        new_weights,
        new_momentum,
        new_averages,
        new_norm_params,
        new_norm_momentum,
        new_norm_averages,
        grad_norm,
    )


def solution(mesh):
    return jax.shard_map(
        local,
        mesh=mesh,
        in_specs=(
            P("dp", None, None),
            P("dp", None, None),
            P("dp", None),
            P("dp"),
            P("dp"),
            P("dp", None),
            P(),
            P(("tower", "dp"), None),
            P(),
            P(("tower", "dp"), None),
            P(),
            P(("tower", "dp"), None),
            P(),
        ),
        out_specs=(
            P(("tower", "dp"), None),
            P(),
            P("dp", None, "tower"),
            P(("tower", "dp"), None),
            P(("tower", "dp"), None),
            P(("tower", "dp"), None),
            P(),
            P(),
            P(),
            P(),
        ),
        check_vma=False,
    )
```
